128 devices in a mesh: runner: 8 (over z, core), tile: 16 (over y, x).
Axes of the slice: x: 4, y: 4, z: 4, core: 2. Of those that a mesh axis runs over, the one named last changes fastest.
Arguments:
- prior_mean_fields: float32 [3, 128, 512], P(None, 'tile'), may hold values from -0.2 to 0.2
- ensemble_deviations: float32 [256, 3, 128, 512], P('runner', None, 'tile'), may hold values from -0.75 to 0.75
- obs_cell: int32 [16, 8, 256], P('tile', 'runner'), may hold values from 0 to 1535
- obs_value: float32 [16, 8, 256], P('tile', 'runner'), may hold values from -3 to 3
- obs_var: float32 [16, 8, 256], P('tile', 'runner'), may hold values from 0.02 to 0.2
Outputs:
- advanced: float32 [256, 3, 128, 512], P('runner', None, 'tile')
The draws below stay inside these ranges and needn't reach their ends.
Inputs may be any that keep to these rules, and one draw needn't show every extreme that they name: obs_cell[t, s, o] numbers a value of slab (t, s) as field * 512 + row within the slab * 512 + column.
All inputs are finite; a program needn't handle non-finite values.
Results may differ from the reference program's by a relative error of at most 0.0001.
Values sent between devices are 32-bit elements; how exact they have to be, the bound alone decides.
No kernel may reach another device: no remote copies, remote signals or barrier semaphores. Data moves between devices by JAX's collectives and lax.ppermute only.
A program may use at most 128 MiB of HBM per device.

```python
import math
import jax
import jax.numpy as jnp
from jax import lax

RUNNER_ENSEMBLE = 32
MESH_WIDTH_CELLS = 512
OBS = 256
DB_ITERS = 3
ENSEMBLE_SIZE = 256
MESH_LATITUDES = 128
BAND_LATITUDES = 1
N_RUNNER = 8
N_TILE = 16


def plant(entries, own_key, smallest, high):
    index_at = [jax.random.randint(jax.random.fold_in(own_key, axis), (), 0, length) for axis, length in enumerate(entries.shape)]
    widest = entries.shape.index(max(entries.shape))
    neighbour = index_at[:widest] + [(index_at[widest] + 1) % entries.shape[widest]] + index_at[widest + 1:]
    return entries.at[tuple(index_at)].set(smallest).at[tuple(neighbour)].set(high)


def levels(rng, dims, split, least, top_value):
    level = 1.0
    for axis_at, parts in split:
        draws = jax.random.uniform(jax.random.fold_in(jax.random.fold_in(rng, 6), axis_at), (parts,), jnp.float32, least / len(split), top_value / len(split))
        level = level * jnp.repeat(jnp.exp(draws), dims[axis_at] // parts).reshape((-1,) + (1,) * (len(dims) - 1 - axis_at))
    return level


def normal_values(rng, shape, spread, bound, shards=(), held_as=jnp.bfloat16):
    factor_of = levels(rng, shape, shards, -0.22, 0.18) if shards else 1.0
    result = jax.random.normal(rng, shape, jnp.float32) * spread * factor_of
    return jnp.minimum(jnp.maximum(result, -bound), bound).astype(held_as)


def setup_inputs(seed: int = 0) -> dict:
    key_of = jax.random.split(jax.random.key(seed), 6)
    return {
        "prior_mean_fields": jnp.clip(jax.random.uniform(key_of[0], (3, MESH_LATITUDES, MESH_WIDTH_CELLS), jnp.float32, -0.2, 0.2) * levels(key_of[0], (3, MESH_LATITUDES, MESH_WIDTH_CELLS), ((1, 16),), -0.4, 0.0), -0.2, 0.2),
        "ensemble_deviations": normal_values(key_of[1], (ENSEMBLE_SIZE, 3, MESH_LATITUDES, MESH_WIDTH_CELLS), 0.05, 0.75, ((0, 8), (2, 16)), jnp.float32),
        "obs_cell": plant(jax.random.randint(key_of[2], (N_TILE, N_RUNNER, OBS), 0, 3 * BAND_LATITUDES * MESH_WIDTH_CELLS), jax.random.fold_in(key_of[2], 1), 0, (3 * BAND_LATITUDES * MESH_WIDTH_CELLS) - 1).astype(jnp.int32),
        "obs_value": normal_values(key_of[3], (N_TILE, N_RUNNER, OBS), 0.2, 3.0, ((0, 16), (1, 8)), jnp.float32),
        "obs_var": jnp.clip(jnp.exp(math.log(0.2) - 2.3025851 * jax.random.uniform(key_of[4], (N_TILE, N_RUNNER, OBS), jnp.float32) ** levels(key_of[4], (N_TILE, N_RUNNER, OBS), ((0, 16), (1, 8)), -0.2, 0.2)), 0.02, 0.2),
    }


TIME_STEP = 0.25
CORIOLIS = 0.2

def along_x(field):
    return (8.0 * (jnp.roll(field, -1, -1) - jnp.roll(field, 1, -1)) - (jnp.roll(field, -2, -1) - jnp.roll(field, 2, -1))) / 12.0

def along_y(padded):
    return (8.0 * (padded[:, 3:-1] - padded[:, 1:-3]) - (padded[:, 4:] - padded[:, :-4])) / 12.0

def tendency_padded(padded):
    height = padded[:, 0]
    east_speed = padded[:, 1]
    north_speed = padded[:, 2]
    column_depth = 1.0 + height
    flux_x = column_depth * east_speed
    flux_y = column_depth * north_speed
    east_mid = east_speed[:, 2:-2]
    north_mid = north_speed[:, 2:-2]
    height_rate = -(along_x(flux_x[:, 2:-2]) + along_y(flux_y))
    east_rate = -(east_mid * along_x(east_mid) + north_mid * along_y(east_speed)) + CORIOLIS * north_mid - along_x(height[:, 2:-2])
    north_rate = -(east_mid * along_x(north_mid) + north_mid * along_y(north_speed)) - CORIOLIS * east_mid - along_y(height)
    return jnp.stack([height_rate, east_rate, north_rate], axis=1)

def runge_kutta_update(state_now, tendency_of):
    slope_one = tendency_of(state_now)
    slope_two = tendency_of(state_now + 0.5 * TIME_STEP * slope_one)
    slope_three = tendency_of(state_now + 0.5 * TIME_STEP * slope_two)
    slope_four = tendency_of(state_now + TIME_STEP * slope_three)
    return state_now + TIME_STEP / 6.0 * (slope_one + 2.0 * slope_two + 2.0 * slope_three + slope_four)

def wrapped_rate_change(state_now):
    padded = jnp.concatenate([state_now[:, :, -2:], state_now, state_now[:, :, :2]], axis=2)
    return tendency_padded(padded)

def symmetric_inverse(matrix, identity):
    sym = 0.5 * (matrix + matrix.T)
    return jax.scipy.linalg.cho_solve((jnp.linalg.cholesky(sym), True), identity)

def inverse_root(matrix, iterations):
    identity = jnp.eye(matrix.shape[0], dtype=matrix.dtype)
    square_root = matrix
    inverse_part = identity
    for _ in range(iterations):
        inv_square = symmetric_inverse(square_root, identity)
        inv_inverse = symmetric_inverse(inverse_part, identity)
        square_root, inverse_part = (0.5 * (square_root + inv_inverse), 0.5 * (inverse_part + inv_square))
    return inverse_part

def make_transform(gram_matrix, innovation, ensemble):
    identity = jnp.eye(ensemble, dtype=gram_matrix.dtype)
    matrix = identity + gram_matrix / (ensemble - 1.0)
    root = inverse_root(matrix, DB_ITERS)
    inner = jnp.dot(root, innovation, precision=lax.Precision.HIGHEST)
    weights = jnp.dot(root, inner, precision=lax.Precision.HIGHEST) / (ensemble - 1.0)
    return root + weights[:, None]

def correct_with_observations(flat_state, columns):
    member_mean = jnp.mean(flat_state, axis=0)
    return member_mean + jnp.einsum('kc,km->mc', flat_state - member_mean, columns, precision=lax.Precision.HIGHEST)

def reference(prior_mean_fields, ensemble_deviations, obs_cell, obs_value, obs_var):
    ensemble_subsets = ensemble_deviations.reshape(N_RUNNER, RUNNER_ENSEMBLE, 3, MESH_LATITUDES, MESH_WIDTH_CELLS)
    integrate_ensemble_trajectory = lax.map(lambda runner_ensemble_subset: runge_kutta_update(prior_mean_fields[None] + runner_ensemble_subset, wrapped_rate_change), ensemble_subsets)
    integrate_ensemble_trajectory = integrate_ensemble_trajectory.reshape(ENSEMBLE_SIZE, 3, MESH_LATITUDES, MESH_WIDTH_CELLS)
    band_with_margins = integrate_ensemble_trajectory.reshape(ENSEMBLE_SIZE, 3, N_TILE, N_RUNNER, BAND_LATITUDES, MESH_WIDTH_CELLS).transpose(2, 3, 0, 1, 4, 5)
    band_with_margins = band_with_margins.reshape(N_TILE, N_RUNNER, ENSEMBLE_SIZE, 3 * BAND_LATITUDES * MESH_WIDTH_CELLS)
    picked = jnp.take_along_axis(band_with_margins, jnp.broadcast_to(obs_cell[:, :, None, :], (N_TILE, N_RUNNER, ENSEMBLE_SIZE, OBS)), axis=3)
    mean_obs = jnp.mean(picked, axis=2)
    anomaly = picked - mean_obs[:, :, None, :]
    scaled = anomaly / obs_var[:, :, None, :]
    gram_matrix = jnp.einsum('tsko,tslo->kl', scaled, anomaly, precision=lax.Precision.HIGHEST)
    innovation = jnp.einsum('tsko,tso->k', scaled, obs_value - mean_obs, precision=lax.Precision.HIGHEST)
    ensemble_mixing_matrix = make_transform(gram_matrix, innovation, ENSEMBLE_SIZE)
    updated_posterior_fields = correct_with_observations(integrate_ensemble_trajectory.reshape(ENSEMBLE_SIZE, -1), ensemble_mixing_matrix).reshape(N_RUNNER, RUNNER_ENSEMBLE, 3, MESH_LATITUDES, MESH_WIDTH_CELLS)
    advanced = lax.map(lambda runner_ensemble_subset: runner_ensemble_subset + TIME_STEP * wrapped_rate_change(runner_ensemble_subset), updated_posterior_fields)
    return advanced.reshape(ENSEMBLE_SIZE, 3, MESH_LATITUDES, MESH_WIDTH_CELLS)
```

```python
import functools
import math

import jax
import jax.numpy as jnp
from jax import lax
from jax.experimental import pallas as pl
from jax.experimental.pallas import tpu as pltpu
from jax.sharding import PartitionSpec as P

TIME_STEP = 0.25
CORIOLIS = 0.2
LANES = 128
ROOT2 = math.sqrt(2.0)
POLE_LOW = 3.0 - 2.0 * ROOT2
POLE_HIGH = 3.0 + 2.0 * ROOT2
SHIFT = (0.0, 1.0, POLE_LOW, POLE_HIGH)
ROOT_CONST = 0.125
ROOT_COEF = (
    0.125,
    0.5,
    2.0 * (1.0 - POLE_LOW) / (POLE_HIGH - POLE_LOW),
    2.0 * (POLE_HIGH - 1.0) / (POLE_HIGH - POLE_LOW),
)
BLOCK = 32


def start_kernel(prior_ref, dev_ref, out_ref):
    members, fields, rows, width = dev_ref.shape
    for m in range(members):
        for f in range(fields):
            for cb in range(width // LANES):
                at = ((m * fields + f) * (width // LANES) + cb) * rows
                lanes = slice(cb * LANES, (cb + 1) * LANES)
                out_ref[at : at + rows, :] = dev_ref[m, f, :, lanes] + prior_ref[f, :, lanes]


def roll_x(field, shift):
    return pltpu.roll(field, shift % field.shape[-1], axis=field.ndim - 1)


def along_x(field):
    return (8.0 / 12.0) * (roll_x(field, -1) - roll_x(field, 1)) - (1.0 / 12.0) * (
        roll_x(field, -2) - roll_x(field, 2)
    )


def along_y(low2, low1, high1, high2):
    return (8.0 / 12.0) * (high1 - low1) - (1.0 / 12.0) * (high2 - low2)


def tendency(load):
    h, u, v = (load(f, 0) for f in range(3))
    hs, us, vs = ([load(f, s) for s in (-2, -1, 1, 2)] for f in range(3))
    flux_y = [(1.0 + a) * b for a, b in zip(hs, vs)]
    height = -(along_x((1.0 + h) * u) + along_y(*flux_y))
    east = -(u * along_x(u) + v * along_y(*us)) + CORIOLIS * v - along_x(h)
    north = -(u * along_x(v) + v * along_y(*vs)) - CORIOLIS * u - along_y(*hs)
    return height, east, north


def runge_kutta_kernel(in_ref, out_ref, cur_ref, acc_ref, *, tiles, members, blocks):
    per = 3 * blocks
    grid_rows = tiles * 8

    def join(parts):
        return jnp.concatenate(parts, axis=1)

    def member_step(m, _):
        def start_of(t, f):
            return join(
                [in_ref[pl.ds(((t * members + m) * per + f * blocks + cb) * 8, 8), :] for cb in range(blocks)]
            )

        def put(side, t, f, value):
            for cb in range(blocks):
                cur_ref[side, f * blocks + cb, pl.ds(8 + t * 8, 8), :] = value[
                    :, cb * LANES : (cb + 1) * LANES
                ]

        def wrap(side):
            for j in range(per):
                cur_ref[side, j, 0:8, :] = cur_ref[side, j, grid_rows : grid_rows + 8, :]
                cur_ref[side, j, grid_rows + 8 : grid_rows + 16, :] = cur_ref[side, j, 8:16, :]

        def fill(t, _):
            for f in range(3):
                put(0, t, f, start_of(t, f))
            return 0

        lax.fori_loop(0, tiles, fill, 0)
        wrap(0)
        for stage in range(4):
            side = stage % 2

            def block_step(t, _, stage=stage, side=side):
                def load(f, shift):
                    return join(
                        [cur_ref[side, f * blocks + cb, pl.ds(8 + t * 8 + shift, 8), :] for cb in range(blocks)]
                    )

                slopes = tendency(load)
                for f in range(3):
                    start = start_of(t, f)
                    weight = TIME_STEP / 6.0 * (1.0 if stage in (0, 3) else 2.0)
                    rows = pl.ds(t * 8, 8)
                    base = start if stage == 0 else acc_ref[f, rows, :]
                    total = base + weight * slopes[f]
                    if stage < 3:
                        acc_ref[f, rows, :] = total
                        step = TIME_STEP * (1.0 if stage == 2 else 0.5)
                        put(1 - side, t, f, start + step * slopes[f])
                    else:
                        for cb in range(blocks):
                            at = t * (members * per) + m * per + f * blocks + cb
                            out_ref[pl.ds(at, 8, stride=tiles * members * per), :] = total[
                                :, cb * LANES : (cb + 1) * LANES
                            ]
                return 0

            lax.fori_loop(0, tiles, block_step, 0)
            if stage < 3:
                wrap(1 - side)
        return 0

    lax.fori_loop(0, members, member_step, 0)


def gram_kernel(in_ref, cell_ref, value_ref, var_ref, pack_ref, dev_ref, mean_ref, *, ensemble, per):
    cells = cell_ref[...]
    inv_var = 1.0 / var_ref[...]
    val_w = value_ref[...] * inv_var
    lane = lax.broadcasted_iota(jnp.int32, (cells.shape[0], LANES), 1)
    total = jnp.zeros((ensemble + 8, ensemble), jnp.float32)
    for pair in range(per // 2):
        devs, lefts = [], []
        for j in (2 * pair, 2 * pair + 1):
            hit = cells == lane + j * LANES
            w = jnp.sum(jnp.where(hit, inv_var, 0.0), axis=0, keepdims=True)
            vw = jnp.sum(jnp.where(hit, val_w, 0.0), axis=0, keepdims=True)
            full = in_ref[pl.ds(j, ensemble, stride=per), :]
            mean = jnp.sum(full, axis=0, keepdims=True) * (1.0 / ensemble)
            dev = full - mean
            dev_ref[:, j * LANES : (j + 1) * LANES] = dev
            mean_ref[:, j * LANES : (j + 1) * LANES] = jnp.broadcast_to(mean, (8, LANES))
            devs.append(dev)
            z = jnp.broadcast_to(vw - mean * w, (8, LANES))
            lefts.append(jnp.concatenate([dev * w, z], axis=0))
        total = total + lax.dot_general(
            jnp.concatenate(lefts, axis=1),
            jnp.concatenate(devs, axis=1),
            (((1,), (1,)), ((), ())),
            precision=lax.Precision.HIGHEST,
            preferred_element_type=jnp.float32,
        )
    half = ensemble // 2
    sub = lax.broadcasted_iota(jnp.int32, (half, LANES), 0)
    for a in range(2):
        for cb in range(2):
            pack_ref[pl.ds(a * 2 + cb, half, stride=5), :] = total[
                a * half : (a + 1) * half, cb * LANES : (cb + 1) * LANES
            ]
    inn = total[ensemble : ensemble + 1, :]
    pack_ref[pl.ds(4, half, stride=5), :] = jnp.where(
        sub == 0,
        jnp.broadcast_to(inn[:, :LANES], (half, LANES)),
        jnp.where(sub == 1, jnp.broadcast_to(inn[:, LANES:], (half, LANES)), 0.0),
    )


def piece_sum_kernel(in_ref, out_ref):
    count = in_ref.shape[0] // 5
    for q in range(5):
        total = jnp.sum(in_ref[pl.ds(q, count, stride=5), :], axis=0, keepdims=True)
        out_ref[pl.ds(q, count, stride=5), :] = jnp.broadcast_to(total, (count, LANES))


def split3(x):
    hi = x.astype(jnp.bfloat16)
    rest = x - hi.astype(jnp.float32)
    mid = rest.astype(jnp.bfloat16)
    low = (rest - mid.astype(jnp.float32)).astype(jnp.bfloat16)
    return hi, mid, low


def packed_inverse(packed, group):
    lane = lax.broadcasted_iota(jnp.int32, packed.shape, 1)
    sub = lax.broadcasted_iota(jnp.int32, packed.shape, 0)
    within = lane % group
    first = lane - within
    for k in range(group):
        column = jnp.take_along_axis(packed, first + k, axis=1)
        row = jnp.broadcast_to(packed[k : k + 1, :], packed.shape)
        pivot = jnp.broadcast_to(column[k : k + 1, :], packed.shape)
        inv = 1.0 / pivot
        row = jnp.where(within == k, -1.0, row) * inv
        swept = jnp.where(within == k, 0.0, packed) - column * row
        packed = jnp.where(sub == k, row, swept)
    return -packed


def root_kernel(in_ref, dev_ref, mean_ref, out_ref, work_ref, *, ensemble, per):
    half = ensemble // 2
    n = ensemble
    row_id = lax.broadcasted_iota(jnp.int32, (n, n), 0)
    lane_id = lax.broadcasted_iota(jnp.int32, (n, n), 1)
    diag = row_id == lane_id
    gram = jnp.concatenate(
        [
            jnp.concatenate([in_ref[pl.ds(a * 2 + cb, half, stride=5), :] for cb in range(2)], axis=1)
            for a in range(2)
        ],
        axis=0,
    )
    matrix = gram * (1.0 / (ensemble - 1.0))
    for s, shift in enumerate(SHIFT):
        work_ref[s] = matrix + jnp.where(diag, 1.0 + shift, 0.0)
    shifts = len(SHIFT)
    lane_small = lax.broadcasted_iota(jnp.int32, (BLOCK, LANES), 1)
    lane_wide = lax.broadcasted_iota(jnp.int32, (BLOCK, n), 1)
    row_wide = lax.broadcasted_iota(jnp.int32, (BLOCK, n), 0)
    for k in range(n // BLOCK):
        rows = [work_ref[s, k * BLOCK : (k + 1) * BLOCK, :] for s in range(shifts)]
        near = (k * BLOCK) // LANES * LANES
        packed = jnp.zeros((BLOCK, LANES), jnp.float32)
        for s in range(shifts):
            move = (BLOCK * s - (k * BLOCK - near)) % LANES
            piece = rows[s][:, near : near + LANES]
            if move:
                piece = pltpu.roll(piece, move, axis=1)
            packed = jnp.where(lane_small // BLOCK == s, piece, packed)
        inverse = packed_inverse(packed, BLOCK)
        left = jnp.concatenate(
            [jnp.where(lane_small // BLOCK == s, inverse, 0.0) for s in range(shifts)], axis=0
        )
        own = (lane_wide >= k * BLOCK) & (lane_wide < (k + 1) * BLOCK)
        minus_eye = jnp.where(lane_wide == row_wide + k * BLOCK, -1.0, 0.0)
        bars = [jnp.where(own, minus_eye, r) for r in rows]
        swept = jnp.dot(
            left,
            jnp.concatenate(bars, axis=0),
            precision=lax.Precision.HIGHEST,
            preferred_element_type=jnp.float32,
        )
        for s in range(shifts):
            z = swept[s * BLOCK : (s + 1) * BLOCK, :]
            y1, y2, y3 = split3(jnp.where(own, 0.0, z))
            r1, r2, r3 = split3(bars[s])
            update = lax.dot_general(
                jnp.concatenate([y1, y1, y2, y2, y1, y3], axis=0),
                jnp.concatenate([r1, r2, r1, r2, r3, r1], axis=0),
                (((0,), (0,)), ((), ())),
                preferred_element_type=jnp.float32,
            )
            own_all = (lane_id >= k * BLOCK) & (lane_id < (k + 1) * BLOCK)
            work_ref[s] = jnp.where(own_all, 0.0, work_ref[s]) - update
            work_ref[s, k * BLOCK : (k + 1) * BLOCK, :] = z
    root = jnp.where(diag, ROOT_CONST, 0.0)
    for s in range(shifts):
        root = root - ROOT_COEF[s] * work_ref[s]
    innovation = jnp.concatenate([in_ref[4:5, :], in_ref[9:10, :]], axis=1)
    inner = jnp.sum(root * innovation, axis=1, keepdims=True)
    weights = jnp.sum(root * inner, axis=0, keepdims=True) * (1.0 / (ensemble - 1.0))
    mixing = root + weights
    for pair in range(per // 2):
        lanes = slice(pair * 2 * LANES, (pair + 1) * 2 * LANES)
        mixed = jnp.dot(
            mixing,
            dev_ref[:, lanes],
            precision=lax.Precision.HIGHEST,
            preferred_element_type=jnp.float32,
        ) + mean_ref[0:1, lanes]
        for i in range(2):
            out_ref[pl.ds(2 * pair + i, ensemble, stride=per), :] = mixed[:, i * LANES : (i + 1) * LANES]


def advance_kernel(main_ref, low_ref, high_ref, out_ref, buf_ref, *, members, per):
    blocks = per // 3
    stride = main_ref.shape[0] // 8
    first = pl.program_id(0) * members

    def one(i, _):
        m = first + i
        for j in range(per):
            buf_ref[j, 8:16, :] = main_ref[pl.ds(m * per + j, 8, stride=stride), :]
            for r in range(2):
                buf_ref[j, 6 + r : 7 + r, :] = low_ref[pl.ds(r * stride + m * per + j, 1), :]
                buf_ref[j, 16 + r : 17 + r, :] = high_ref[pl.ds(r * stride + m * per + j, 1), :]

        def load(f, shift):
            return jnp.concatenate(
                [buf_ref[f * blocks + cb, 8 + shift : 16 + shift, :] for cb in range(blocks)], axis=1
            )

        slopes = tendency(load)
        for f in range(3):
            out_ref[i, f] = load(f, 0) + TIME_STEP * slopes[f]
        return 0

    lax.fori_loop(0, members, one, 0)


VMEM = pl.BlockSpec(memory_space=pltpu.VMEM)


def f32(*shape):
    return jax.ShapeDtypeStruct(shape, jnp.float32)


def make_start(prior, deviations):
    members, fields, rows, width = deviations.shape
    step = 8
    return pl.pallas_call(
        start_kernel,
        grid=(members // step,),
        in_specs=[
            pl.BlockSpec((fields, rows, width), lambda i: (0, 0, 0)),
            pl.BlockSpec((step, fields, rows, width), lambda i: (i, 0, 0, 0)),
        ],
        out_specs=pl.BlockSpec((step * fields * rows * width // LANES, LANES), lambda i: (i, 0)),
        out_shape=f32(members * fields * rows * width // LANES, LANES),
        name="start",
    )(prior, deviations)


def runge_kutta(rows, tiles, members, blocks):
    per = 3 * blocks
    return pl.pallas_call(
        functools.partial(runge_kutta_kernel, tiles=tiles, members=members, blocks=blocks),
        in_specs=[VMEM],
        out_specs=VMEM,
        out_shape=f32(*rows.shape),
        scratch_shapes=[
            pltpu.VMEM((2, per, tiles * 8 + 16, LANES), jnp.float32),
            pltpu.VMEM((3, tiles * 8, blocks * LANES), jnp.float32),
        ],
        name="runge_kutta",
    )(rows)


def gram_pieces(rows, cell, value, var, ensemble, per):
    return pl.pallas_call(
        functools.partial(gram_kernel, ensemble=ensemble, per=per),
        in_specs=[VMEM] * 4,
        out_specs=[VMEM] * 3,
        out_shape=[f32(ensemble // 2 * 5, LANES), f32(ensemble, per * LANES), f32(8, per * LANES)],
        name="gram",
    )(rows, cell, value, var)


def piece_sum(pieces):
    return pl.pallas_call(
        piece_sum_kernel, in_specs=[VMEM], out_specs=VMEM, out_shape=f32(*pieces.shape), name="piece_sum"
    )(pieces)


def analyse(pieces, dev, mean, ensemble, per):
    return pl.pallas_call(
        functools.partial(root_kernel, ensemble=ensemble, per=per),
        in_specs=[VMEM] * 3,
        out_specs=VMEM,
        out_shape=f32(ensemble * per, LANES),
        scratch_shapes=[pltpu.VMEM((len(SHIFT), ensemble, ensemble), jnp.float32)],
        name="analyse",
    )(pieces, dev, mean)


def advance(main, low, high, members, per):
    step = 8
    return pl.pallas_call(
        functools.partial(advance_kernel, members=step, per=per),
        grid=(members // step,),
        in_specs=[VMEM] * 3,
        out_specs=pl.BlockSpec((step, 3, 8, per // 3 * LANES), lambda i: (i, 0, 0, 0)),
        out_shape=f32(members, 3, 8, per // 3 * LANES),
        scratch_shapes=[pltpu.VMEM((per, 24, LANES), jnp.float32)],
        name="advance",
    )(main, low, high)


def exchange(rows, axes, count):
    moved = lax.all_to_all(rows.reshape(count, -1), axes, 0, 0, tiled=True)
    return moved.reshape(rows.shape)


def per_device(prior_mean_fields, ensemble_deviations, obs_cell, obs_value, obs_var):
    runners, tiles = lax.axis_size("runner"), lax.axis_size("tile")
    members_dev, _, _, width = ensemble_deviations.shape
    blocks = width // LANES
    per = 3 * blocks
    ensemble = members_dev * runners
    whole = ("runner", "tile")
    start = make_start(prior_mean_fields, ensemble_deviations)
    grids = exchange(start, "tile", tiles)
    forecast = runge_kutta(grids, tiles, members_dev // tiles, blocks)
    slab = exchange(forecast, whole, runners * tiles)
    pieces, dev, mean = gram_pieces(
        slab, obs_cell.reshape(-1, 1), obs_value.reshape(-1, 1), obs_var.reshape(-1, 1), ensemble, per
    )
    pieces = exchange(pieces, whole, runners * tiles)
    pieces = exchange(piece_sum(pieces), whole, runners * tiles)
    analysed = exchange(analyse(pieces, dev, mean, ensemble, per), "runner", runners)
    edge = 2 * members_dev * per
    forward = [(i, (i + 1) % tiles) for i in range(tiles)]
    backward = [(target, source) for source, target in forward]
    low = lax.ppermute(analysed[-edge:], "tile", forward)
    high = lax.ppermute(analysed[:edge], "tile", backward)
    return advance(analysed, low, high, members_dev, per)


def solution(mesh):
    placed = (
        P(None, "tile", None),
        P("runner", None, "tile", None),
        P("tile", "runner", None),
        P("tile", "runner", None),
        P("tile", "runner", None),
    )
    return jax.shard_map(
        per_device,
        mesh=mesh,
        in_specs=placed,
        out_specs=P("runner", None, "tile", None),
        check_vma=False,
    )
```

```python
import functools
import math

import jax
import jax.numpy as jnp
from jax import lax
from jax.experimental import pallas as pl
from jax.experimental.pallas import tpu as pltpu
from jax.sharding import PartitionSpec as P

TIME_STEP = 0.25
CORIOLIS = 0.2
LANES = 128
ROOT2 = math.sqrt(2.0)
POLE_LOW = 3.0 - 2.0 * ROOT2
POLE_HIGH = 3.0 + 2.0 * ROOT2
SHIFT = (0.0, 1.0, POLE_LOW, POLE_HIGH)
ROOT_CONST = 0.125
ROOT_COEF = (
    0.125,
    0.5,
    2.0 * (1.0 - POLE_LOW) / (POLE_HIGH - POLE_LOW),
    2.0 * (POLE_HIGH - 1.0) / (POLE_HIGH - POLE_LOW),
)
BLOCK = 32
PANEL = 16


def start_kernel(prior_ref, dev_ref, out_ref):
    members, fields, rows, width = dev_ref.shape
    for m in range(members):
        for f in range(fields):
            for cb in range(width // LANES):
                at = ((m * fields + f) * (width // LANES) + cb) * rows
                lanes = slice(cb * LANES, (cb + 1) * LANES)
                out_ref[at : at + rows, :] = dev_ref[m, f, :, lanes] + prior_ref[f, :, lanes]


def roll_x(field, shift):
    return pltpu.roll(field, shift % field.shape[-1], axis=field.ndim - 1)


def along_x(field):
    return (roll_x(field, -1) - roll_x(field, 1)) - 0.125 * (roll_x(field, -2) - roll_x(field, 2))


def along_y(load, f):
    return (load(f, 1) - load(f, -1)) - 0.125 * (load(f, 2) - load(f, -2))


SLOPE = 8.0 / 12.0


def tendency(load):
    h, u, v = (load(f, 0) for f in range(3))
    height = -SLOPE * (along_x((1.0 + h) * u) + along_y(load, 3))
    east = CORIOLIS * v - SLOPE * (u * along_x(u) + v * along_y(load, 1) + along_x(h))
    north = -CORIOLIS * u - SLOPE * (u * along_x(v) + v * along_y(load, 2) + along_y(load, 0))
    return height, east, north


UNROLL = 4


def runge_kutta_kernel(in_ref, out_ref, even_ref, odd_ref, acc_ref, *, tiles, members, blocks):
    per = 3 * blocks
    grid_rows = tiles * 8
    sides = (even_ref, odd_ref)

    def split(value):
        return [value[:, cb * LANES : (cb + 1) * LANES] for cb in range(blocks)]

    def every_tile(step):
        def some(i, _):
            for r in range(UNROLL):
                step(i * UNROLL + r)
            return 0

        lax.fori_loop(0, tiles // UNROLL, some, 0)

    def member_step(m, _):
        def start_of(t, f):
            return jnp.concatenate(
                [in_ref[pl.ds(((t * members + m) * per + f * blocks + cb) * 8, 8), :] for cb in range(blocks)],
                axis=1,
            )

        def put(ref, t, values):
            flux = (1.0 + values[0]) * values[2]
            for f, value in enumerate((*values, flux)):
                for cb, part in enumerate(split(value)):
                    ref[f * blocks + cb, pl.ds(8 + t * 8, 8), :] = part

        def wrap(ref):
            for j in range(4 * blocks):
                ref[j, 0:8, :] = ref[j, grid_rows : grid_rows + 8, :]
                ref[j, grid_rows + 8 : grid_rows + 16, :] = ref[j, 8:16, :]

        every_tile(lambda t: put(even_ref, t, [start_of(t, f) for f in range(3)]))
        wrap(even_ref)
        for stage in range(4):
            here, there = sides[stage % 2], sides[1 - stage % 2]

            def step(t, stage=stage, here=here, there=there):
                def load(f, shift):
                    return jnp.concatenate(
                        [here[f * blocks + cb, pl.ds(8 + t * 8 + shift, 8), :] for cb in range(blocks)],
                        axis=1,
                    )

                slopes = tendency(load)
                rows = pl.ds(t * 8, 8)
                nexts = []
                for f in range(3):
                    start = start_of(t, f)
                    weight = TIME_STEP / 6.0 * (1.0 if stage in (0, 3) else 2.0)
                    total = (start if stage == 0 else acc_ref[f, rows, :]) + weight * slopes[f]
                    if stage < 3:
                        acc_ref[f, rows, :] = total
                        nexts.append(start + TIME_STEP * (1.0 if stage == 2 else 0.5) * slopes[f])
                    else:
                        for cb, part in enumerate(split(total)):
                            at = t * (members * per) + m * per + f * blocks + cb
                            out_ref[pl.ds(at, 8, stride=tiles * members * per), :] = part
                if stage < 3:
                    put(there, t, nexts)

            every_tile(step)
            if stage < 3:
                wrap(there)
        return 0

    lax.fori_loop(0, members, member_step, 0)


def gram_kernel(in_ref, cell_ref, value_ref, var_ref, pack_ref, dev_ref, mean_ref, *, ensemble, per):
    cells = cell_ref[...]
    inv_var = 1.0 / var_ref[...]
    val_w = value_ref[...] * inv_var
    lane = lax.broadcasted_iota(jnp.int32, (cells.shape[0], LANES), 1)
    total = jnp.zeros((ensemble + 8, ensemble), jnp.float32)
    for pair in range(per // 2):
        devs, lefts = [], []
        for j in (2 * pair, 2 * pair + 1):
            hit = cells == lane + j * LANES
            w = jnp.sum(jnp.where(hit, inv_var, 0.0), axis=0, keepdims=True)
            vw = jnp.sum(jnp.where(hit, val_w, 0.0), axis=0, keepdims=True)
            full = in_ref[pl.ds(j, ensemble, stride=per), :]
            mean = jnp.sum(full, axis=0, keepdims=True) * (1.0 / ensemble)
            dev = full - mean
            dev_ref[:, j * LANES : (j + 1) * LANES] = dev
            mean_ref[:, j * LANES : (j + 1) * LANES] = jnp.broadcast_to(mean, (8, LANES))
            devs.append(dev)
            z = jnp.broadcast_to(vw - mean * w, (8, LANES))
            lefts.append(jnp.concatenate([dev * w, z], axis=0))
        total = total + lax.dot_general(
            jnp.concatenate(lefts, axis=1),
            jnp.concatenate(devs, axis=1),
            (((1,), (1,)), ((), ())),
            precision=lax.Precision.HIGHEST,
            preferred_element_type=jnp.float32,
        )
    half = ensemble // 2
    sub = lax.broadcasted_iota(jnp.int32, (half, LANES), 0)
    for a in range(2):
        for cb in range(2):
            pack_ref[pl.ds(a * 2 + cb, half, stride=5), :] = total[
                a * half : (a + 1) * half, cb * LANES : (cb + 1) * LANES
            ]
    inn = total[ensemble : ensemble + 1, :]
    pack_ref[pl.ds(4, half, stride=5), :] = jnp.where(
        sub == 0,
        jnp.broadcast_to(inn[:, :LANES], (half, LANES)),
        jnp.where(sub == 1, jnp.broadcast_to(inn[:, LANES:], (half, LANES)), 0.0),
    )


def piece_sum_kernel(in_ref, out_ref):
    count = in_ref.shape[0] // 5
    for q in range(5):
        total = jnp.sum(in_ref[pl.ds(q, count, stride=5), :], axis=0, keepdims=True)
        out_ref[pl.ds(q, count, stride=5), :] = jnp.broadcast_to(total, (count, LANES))


def split3(x):
    hi = x.astype(jnp.bfloat16)
    rest = x - hi.astype(jnp.float32)
    mid = rest.astype(jnp.bfloat16)
    low = (rest - mid.astype(jnp.float32)).astype(jnp.bfloat16)
    return hi, mid, low


def packed_inverse(packed, group):
    shape = (8, LANES)
    lane = lax.broadcasted_iota(jnp.int32, shape, 1)
    sub = lax.broadcasted_iota(jnp.int32, shape, 0)
    within = lane % group
    first = lane - within
    count = group // 8
    rows = [packed[8 * i : 8 * i + 8, :] for i in range(count)]

    def spread(parts, k):
        return jnp.broadcast_to(parts[k // 8][k % 8 : k % 8 + 1, :], shape)

    def sweep(parts, column, k, row):
        out = [part - c * row for part, c in zip(parts, column)]
        out[k // 8] = jnp.where(sub == k % 8, row, out[k // 8])
        return out

    for k0 in range(0, group, PANEL):
        panel = range(k0, k0 + PANEL)
        columns = {k: [jnp.take_along_axis(part, first + k, axis=1) for part in rows] for k in panel}
        for k in panel:
            column = columns.pop(k)
            inv = 1.0 / spread(column, k)
            for j in columns:
                columns[j] = sweep(columns[j], column, k, spread(columns[j], k) * inv)
            row = jnp.where(within == k, -1.0, spread(rows, k)) * inv
            rows = sweep([jnp.where(within == k, 0.0, part) for part in rows], column, k, row)
    return jnp.concatenate(rows, axis=0)


def root_kernel(in_ref, dev_ref, mean_ref, out_ref, work_ref, *, ensemble, per):
    half = ensemble // 2
    n = ensemble
    row_id = lax.broadcasted_iota(jnp.int32, (n, n), 0)
    lane_id = lax.broadcasted_iota(jnp.int32, (n, n), 1)
    diag = row_id == lane_id
    gram = jnp.concatenate(
        [
            jnp.concatenate([in_ref[pl.ds(a * 2 + cb, half, stride=5), :] for cb in range(2)], axis=1)
            for a in range(2)
        ],
        axis=0,
    )
    matrix = gram * (1.0 / (ensemble - 1.0))
    for s, shift in enumerate(SHIFT):
        work_ref[s] = matrix + jnp.where(diag, 1.0 + shift, 0.0)
    shifts = len(SHIFT)
    lane_small = lax.broadcasted_iota(jnp.int32, (BLOCK, LANES), 1)
    lane_wide = lax.broadcasted_iota(jnp.int32, (BLOCK, n), 1)
    row_wide = lax.broadcasted_iota(jnp.int32, (BLOCK, n), 0)
    for k in range(n // BLOCK):
        rows = [work_ref[s, k * BLOCK : (k + 1) * BLOCK, :] for s in range(shifts)]
        near = (k * BLOCK) // LANES * LANES
        packed = jnp.zeros((BLOCK, LANES), jnp.float32)
        for s in range(shifts):
            move = (BLOCK * s - (k * BLOCK - near)) % LANES
            piece = rows[s][:, near : near + LANES]
            if move:
                piece = pltpu.roll(piece, move, axis=1)
            packed = jnp.where(lane_small // BLOCK == s, piece, packed)
        inverse = packed_inverse(packed, BLOCK)
        left = jnp.concatenate(
            [jnp.where(lane_small // BLOCK == s, -inverse, 0.0) for s in range(shifts)], axis=0
        )
        own = (lane_wide >= k * BLOCK) & (lane_wide < (k + 1) * BLOCK)
        minus_eye = jnp.where(lane_wide == row_wide + k * BLOCK, -1.0, 0.0)
        bars = [jnp.where(own, minus_eye, r) for r in rows]
        swept = jnp.dot(
            left,
            jnp.concatenate(bars, axis=0),
            precision=lax.Precision.HIGHEST,
            preferred_element_type=jnp.float32,
        )
        for s in range(shifts):
            z = swept[s * BLOCK : (s + 1) * BLOCK, :]
            y1, y2, y3 = split3(jnp.where(own, 0.0, z))
            r1, r2, r3 = split3(bars[s])
            update = lax.dot_general(
                jnp.concatenate([y1, y1, y2, y2, y1, y3], axis=0),
                jnp.concatenate([r1, r2, r1, r2, r3, r1], axis=0),
                (((0,), (0,)), ((), ())),
                preferred_element_type=jnp.float32,
            )
            own_all = (lane_id >= k * BLOCK) & (lane_id < (k + 1) * BLOCK)
            work_ref[s] = jnp.where(own_all, 0.0, work_ref[s]) - update
            work_ref[s, k * BLOCK : (k + 1) * BLOCK, :] = z
    root = jnp.where(diag, ROOT_CONST, 0.0)
    for s in range(shifts):
        root = root - ROOT_COEF[s] * work_ref[s]
    innovation = jnp.concatenate([in_ref[4:5, :], in_ref[9:10, :]], axis=1)
    inner = jnp.sum(root * innovation, axis=1, keepdims=True)
    weights = jnp.sum(root * inner, axis=0, keepdims=True) * (1.0 / (ensemble - 1.0))
    mixing = root + weights
    for pair in range(per // 2):
        lanes = slice(pair * 2 * LANES, (pair + 1) * 2 * LANES)
        mixed = jnp.dot(
            mixing,
            dev_ref[:, lanes],
            precision=lax.Precision.HIGHEST,
            preferred_element_type=jnp.float32,
        ) + mean_ref[0:1, lanes]
        for i in range(2):
            out_ref[pl.ds(2 * pair + i, ensemble, stride=per), :] = mixed[:, i * LANES : (i + 1) * LANES]


def advance_kernel(main_ref, low_ref, high_ref, out_ref, buf_ref, *, members, per):
    blocks = per // 3
    stride = main_ref.shape[0] // 8
    first = pl.program_id(0) * members

    def one(i, slot):
        m = first + i
        for at, ref, count in ((6, low_ref, 2), (8, main_ref, 8), (16, high_ref, 2)):
            parts = [ref[pl.ds(m * per + j, count, stride=stride), :] for j in range(per)]
            parts += [(1.0 + parts[cb]) * parts[2 * blocks + cb] for cb in range(blocks)]
            for j, part in enumerate(parts):
                buf_ref[slot, j, at : at + count, :] = part

        def load(f, shift):
            return jnp.concatenate(
                [buf_ref[slot, f * blocks + cb, 8 + shift : 16 + shift, :] for cb in range(blocks)], axis=1
            )

        slopes = tendency(load)
        for f in range(3):
            out_ref[i, f] = load(f, 0) + TIME_STEP * slopes[f]

    def some(i, _):
        for r in range(UNROLL):
            one(i * UNROLL + r, r)
        return 0

    lax.fori_loop(0, members // UNROLL, some, 0)


VMEM = pl.BlockSpec(memory_space=pltpu.VMEM)


def f32(*shape):
    return jax.ShapeDtypeStruct(shape, jnp.float32)


def make_start(prior, deviations):
    members, fields, rows, width = deviations.shape
    step = 16
    return pl.pallas_call(
        start_kernel,
        grid=(members // step,),
        in_specs=[
            pl.BlockSpec((fields, rows, width), lambda i: (0, 0, 0)),
            pl.BlockSpec((step, fields, rows, width), lambda i: (i, 0, 0, 0)),
        ],
        out_specs=pl.BlockSpec((step * fields * rows * width // LANES, LANES), lambda i: (i, 0)),
        out_shape=f32(members * fields * rows * width // LANES, LANES),
        name="start",
    )(prior, deviations)


def runge_kutta(rows, tiles, members, blocks):
    per = 3 * blocks
    return pl.pallas_call(
        functools.partial(runge_kutta_kernel, tiles=tiles, members=members, blocks=blocks),
        in_specs=[VMEM],
        out_specs=VMEM,
        out_shape=f32(*rows.shape),
        scratch_shapes=[
            pltpu.VMEM((4 * blocks, tiles * 8 + 16, LANES), jnp.float32),
            pltpu.VMEM((4 * blocks, tiles * 8 + 16, LANES), jnp.float32),
            pltpu.VMEM((3, tiles * 8, blocks * LANES), jnp.float32),
        ],
        name="runge_kutta",
    )(rows)


def gram_pieces(rows, cell, value, var, ensemble, per):
    return pl.pallas_call(
        functools.partial(gram_kernel, ensemble=ensemble, per=per),
        in_specs=[VMEM] * 4,
        out_specs=[VMEM] * 3,
        out_shape=[f32(ensemble // 2 * 5, LANES), f32(ensemble, per * LANES), f32(8, per * LANES)],
        name="gram",
    )(rows, cell, value, var)


def piece_sum(pieces):
    return pl.pallas_call(
        piece_sum_kernel, in_specs=[VMEM], out_specs=VMEM, out_shape=f32(*pieces.shape), name="piece_sum"
    )(pieces)


def analyse(pieces, dev, mean, ensemble, per):
    return pl.pallas_call(
        functools.partial(root_kernel, ensemble=ensemble, per=per),
        in_specs=[VMEM] * 3,
        out_specs=VMEM,
        out_shape=f32(ensemble * per, LANES),
        scratch_shapes=[pltpu.VMEM((len(SHIFT), ensemble, ensemble), jnp.float32)],
        name="analyse",
    )(pieces, dev, mean)


def advance(main, low, high, members, per):
    step = 8
    return pl.pallas_call(
        functools.partial(advance_kernel, members=step, per=per),
        grid=(members // step,),
        in_specs=[VMEM] * 3,
        out_specs=pl.BlockSpec((step, 3, 8, per // 3 * LANES), lambda i: (i, 0, 0, 0)),
        out_shape=f32(members, 3, 8, per // 3 * LANES),
        scratch_shapes=[pltpu.VMEM((UNROLL, per // 3 * 4, 24, LANES), jnp.float32)],
        name="advance",
    )(main, low, high)


def exchange(rows, axes, count):
    moved = lax.all_to_all(rows.reshape(count, -1), axes, 0, 0, tiled=True)
    return moved.reshape(rows.shape)


def per_device(prior_mean_fields, ensemble_deviations, obs_cell, obs_value, obs_var):
    runners, tiles = lax.axis_size("runner"), lax.axis_size("tile")
    members_dev, _, _, width = ensemble_deviations.shape
    blocks = width // LANES
    per = 3 * blocks
    ensemble = members_dev * runners
    whole = ("runner", "tile")
    start = make_start(prior_mean_fields, ensemble_deviations)
    grids = exchange(start, "tile", tiles)
    forecast = runge_kutta(grids, tiles, members_dev // tiles, blocks)
    slab = exchange(forecast, whole, runners * tiles)
    pieces, dev, mean = gram_pieces(
        slab, obs_cell.reshape(-1, 1), obs_value.reshape(-1, 1), obs_var.reshape(-1, 1), ensemble, per
    )
    pieces = exchange(pieces, whole, runners * tiles)
    pieces = exchange(piece_sum(pieces), whole, runners * tiles)
    analysed = exchange(analyse(pieces, dev, mean, ensemble, per), "runner", runners)
    edge = 2 * members_dev * per
    forward = [(i, (i + 1) % tiles) for i in range(tiles)]
    backward = [(target, source) for source, target in forward]
    low = lax.ppermute(analysed[-edge:], "tile", forward)
    high = lax.ppermute(analysed[:edge], "tile", backward)
    return advance(analysed, low, high, members_dev, per)


def solution(mesh):
    placed = (
        P(None, "tile", None),
        P("runner", None, "tile", None),
        P("tile", "runner", None),
        P("tile", "runner", None),
        P("tile", "runner", None),
    )
    return jax.shard_map(
        per_device,
        mesh=mesh,
        in_specs=placed,
        out_specs=P("runner", None, "tile", None),
        check_vma=False,
    )
```

```python
import functools
import math

import jax
import jax.numpy as jnp
from jax import lax
from jax.experimental import pallas as pl
from jax.experimental.pallas import tpu as pltpu
from jax.sharding import PartitionSpec as P

TIME_STEP = 0.25
CORIOLIS = 0.2
LANES = 128
ROOT2 = math.sqrt(2.0)
POLE_LOW = 3.0 - 2.0 * ROOT2
POLE_HIGH = 3.0 + 2.0 * ROOT2
SHIFT = (0.0, 1.0, POLE_LOW, POLE_HIGH)
ROOT_CONST = 0.125
ROOT_COEF = (
    0.125,
    0.5,
    2.0 * (1.0 - POLE_LOW) / (POLE_HIGH - POLE_LOW),
    2.0 * (POLE_HIGH - 1.0) / (POLE_HIGH - POLE_LOW),
)
BLOCK = 32
PANEL = 16
PIECE = 3
SPLIT = 2


def start_kernel(prior_ref, dev_ref, *out_refs):
    members, fields, rows, width = dev_ref.shape
    split = len(out_refs)
    for m in range(members):
        for f in range(fields):
            for cb in range(width // LANES):
                at = ((m // split * fields + f) * (width // LANES) + cb) * rows
                lanes = slice(cb * LANES, (cb + 1) * LANES)
                out_refs[m % split][at : at + rows, :] = dev_ref[m, f, :, lanes] + prior_ref[f, :, lanes]


def roll_x(field, shift):
    return pltpu.roll(field, shift % field.shape[-1], axis=field.ndim - 1)


def along_x(field):
    return (roll_x(field, -1) - roll_x(field, 1)) - 0.125 * (roll_x(field, -2) - roll_x(field, 2))


def along_y(load, f):
    return (load(f, 1) - load(f, -1)) - 0.125 * (load(f, 2) - load(f, -2))


SLOPE = 8.0 / 12.0


def tendency(load):
    h, u, v = (load(f, 0) for f in range(3))
    height = -SLOPE * (along_x((1.0 + h) * u) + along_y(load, 3))
    east = CORIOLIS * v - SLOPE * (u * along_x(u) + v * along_y(load, 1) + along_x(h))
    north = -CORIOLIS * u - SLOPE * (u * along_x(v) + v * along_y(load, 2) + along_y(load, 0))
    return height, east, north


UNROLL = 4


def runge_kutta_kernel(in_ref, out_ref, even_ref, odd_ref, acc_ref, *, tiles, members, blocks):
    per = 3 * blocks
    grid_rows = tiles * 8
    sides = (even_ref, odd_ref)

    def split(value):
        return [value[:, cb * LANES : (cb + 1) * LANES] for cb in range(blocks)]

    def every_tile(step):
        def some(i, _):
            for r in range(UNROLL):
                step(i * UNROLL + r)
            return 0

        lax.fori_loop(0, tiles // UNROLL, some, 0)

    def member_step(m, _):
        def start_of(t, f):
            return jnp.concatenate(
                [in_ref[pl.ds(((t * members + m) * per + f * blocks + cb) * 8, 8), :] for cb in range(blocks)],
                axis=1,
            )

        def put(ref, t, values):
            flux = (1.0 + values[0]) * values[2]
            for f, value in enumerate((*values, flux)):
                for cb, part in enumerate(split(value)):
                    ref[f * blocks + cb, pl.ds(8 + t * 8, 8), :] = part

        def wrap(ref):
            for j in range(4 * blocks):
                ref[j, 0:8, :] = ref[j, grid_rows : grid_rows + 8, :]
                ref[j, grid_rows + 8 : grid_rows + 16, :] = ref[j, 8:16, :]

        every_tile(lambda t: put(even_ref, t, [start_of(t, f) for f in range(3)]))
        wrap(even_ref)
        for stage in range(4):
            here, there = sides[stage % 2], sides[1 - stage % 2]

            def step(t, stage=stage, here=here, there=there):
                def load(f, shift):
                    return jnp.concatenate(
                        [here[f * blocks + cb, pl.ds(8 + t * 8 + shift, 8), :] for cb in range(blocks)],
                        axis=1,
                    )

                slopes = tendency(load)
                rows = pl.ds(t * 8, 8)
                nexts = []
                for f in range(3):
                    start = start_of(t, f)
                    weight = TIME_STEP / 6.0 * (1.0 if stage in (0, 3) else 2.0)
                    total = (start if stage == 0 else acc_ref[f, rows, :]) + weight * slopes[f]
                    if stage < 3:
                        acc_ref[f, rows, :] = total
                        nexts.append(start + TIME_STEP * (1.0 if stage == 2 else 0.5) * slopes[f])
                    else:
                        for cb, part in enumerate(split(total)):
                            at = t * (members * per) + m * per + f * blocks + cb
                            out_ref[pl.ds(at, 8, stride=tiles * members * per), :] = part
                if stage < 3:
                    put(there, t, nexts)

            every_tile(step)
            if stage < 3:
                wrap(there)
        return 0

    lax.fori_loop(0, members, member_step, 0)


def gram_kernel(*refs, split, ensemble, per):
    slabs, (cell_ref, value_ref, var_ref, pack_ref, dev_ref, mean_ref) = refs[:split], refs[split:]
    cells = cell_ref[...]
    inv_var = 1.0 / var_ref[...]
    val_w = value_ref[...] * inv_var
    lane = lax.broadcasted_iota(jnp.int32, (cells.shape[0], LANES), 1)
    total = jnp.zeros((ensemble + 8, ensemble), jnp.float32)
    for pair in range(per // 2):
        devs, lefts = [], []
        for j in (2 * pair, 2 * pair + 1):
            hit = cells == lane + j * LANES
            w = jnp.sum(jnp.where(hit, inv_var, 0.0), axis=0, keepdims=True)
            vw = jnp.sum(jnp.where(hit, val_w, 0.0), axis=0, keepdims=True)
            full = jnp.concatenate([slab[pl.ds(j, ensemble // split, stride=per), :] for slab in slabs], axis=0)
            mean = jnp.sum(full, axis=0, keepdims=True) * (1.0 / ensemble)
            dev = full - mean
            dev_ref[:, j * LANES : (j + 1) * LANES] = dev
            mean_ref[:, j * LANES : (j + 1) * LANES] = jnp.broadcast_to(mean, (8, LANES))
            devs.append(dev)
            z = jnp.broadcast_to(vw - mean * w, (8, LANES))
            lefts.append(jnp.concatenate([dev * w, z], axis=0))
        total = total + lax.dot_general(
            jnp.concatenate(lefts, axis=1),
            jnp.concatenate(devs, axis=1),
            (((1,), (1,)), ((), ())),
            precision=lax.Precision.HIGHEST,
            preferred_element_type=jnp.float32,
        )
    half = ensemble // 2
    sub = lax.broadcasted_iota(jnp.int32, (half, LANES), 0)
    col = lax.broadcasted_iota(jnp.int32, (half, LANES), 1)
    low, high = total[half:ensemble, LANES:], total[:half, :LANES]
    diagonal = jnp.sum(jnp.where(sub == col, low, 0.0), axis=0, keepdims=True)
    inn = total[ensemble : ensemble + 1, :]
    pack_ref[pl.ds(0, half, stride=PIECE), :] = total[:half, LANES:]
    pack_ref[pl.ds(1, half, stride=PIECE), :] = jnp.where(col >= sub, high, low)
    extra = jnp.zeros((half, LANES), jnp.float32)
    for i, row in enumerate((inn[:, :LANES], inn[:, LANES:], diagonal)):
        extra = jnp.where(sub == i, jnp.broadcast_to(row, (half, LANES)), extra)
    pack_ref[pl.ds(2, half, stride=PIECE), :] = extra


def unpack_gram(ref, half):
    sub = lax.broadcasted_iota(jnp.int32, (half, LANES), 0)
    col = lax.broadcasted_iota(jnp.int32, (half, LANES), 1)
    cross = ref[pl.ds(0, half, stride=PIECE), :]
    both = ref[pl.ds(1, half, stride=PIECE), :]
    turned = both.T
    first = jnp.where(col >= sub, both, turned)
    second = jnp.where(col < sub, both, turned)
    second = jnp.where(col == sub, jnp.broadcast_to(ref[2 * PIECE + 2 : 2 * PIECE + 3, :], (half, LANES)), second)
    gram = jnp.concatenate(
        [jnp.concatenate([first, cross], axis=1), jnp.concatenate([cross.T, second], axis=1)], axis=0
    )
    innovation = jnp.concatenate([ref[2:3, :], ref[PIECE + 2 : PIECE + 3, :]], axis=1)
    return gram, innovation


def piece_sum_kernel(in_ref, out_ref):
    count = in_ref.shape[0] // PIECE
    for q in range(PIECE):
        total = jnp.sum(in_ref[pl.ds(q, count, stride=PIECE), :], axis=0, keepdims=True)
        out_ref[pl.ds(q, count, stride=PIECE), :] = jnp.broadcast_to(total, (count, LANES))


def split3(x):
    hi = x.astype(jnp.bfloat16)
    rest = x - hi.astype(jnp.float32)
    mid = rest.astype(jnp.bfloat16)
    low = (rest - mid.astype(jnp.float32)).astype(jnp.bfloat16)
    return hi, mid, low


def packed_inverse(packed, group):
    shape = (8, LANES)
    lane = lax.broadcasted_iota(jnp.int32, shape, 1)
    sub = lax.broadcasted_iota(jnp.int32, shape, 0)
    within = lane % group
    first = lane - within
    count = group // 8
    rows = [packed[8 * i : 8 * i + 8, :] for i in range(count)]

    def spread(parts, k):
        return jnp.broadcast_to(parts[k // 8][k % 8 : k % 8 + 1, :], shape)

    def sweep(parts, column, k, row):
        out = [part - c * row for part, c in zip(parts, column)]
        out[k // 8] = jnp.where(sub == k % 8, row, out[k // 8])
        return out

    for k0 in range(0, group, PANEL):
        panel = range(k0, k0 + PANEL)
        columns = {k: [jnp.take_along_axis(part, first + k, axis=1) for part in rows] for k in panel}
        for k in panel:
            column = columns.pop(k)
            inv = 1.0 / spread(column, k)
            for j in columns:
                columns[j] = sweep(columns[j], column, k, spread(columns[j], k) * inv)
            row = jnp.where(within == k, -1.0, spread(rows, k)) * inv
            rows = sweep([jnp.where(within == k, 0.0, part) for part in rows], column, k, row)
    return jnp.concatenate(rows, axis=0)


def root_kernel(in_ref, dev_ref, mean_ref, *refs, ensemble, per):
    out_refs, work_ref = refs[:-1], refs[-1]
    half = ensemble // 2
    n = ensemble
    row_id = lax.broadcasted_iota(jnp.int32, (n, n), 0)
    lane_id = lax.broadcasted_iota(jnp.int32, (n, n), 1)
    diag = row_id == lane_id
    gram, innovation = unpack_gram(in_ref, half)
    matrix = gram * (1.0 / (ensemble - 1.0))
    for s, shift in enumerate(SHIFT):
        work_ref[s] = matrix + jnp.where(diag, 1.0 + shift, 0.0)
    shifts = len(SHIFT)
    lane_small = lax.broadcasted_iota(jnp.int32, (BLOCK, LANES), 1)
    lane_wide = lax.broadcasted_iota(jnp.int32, (BLOCK, n), 1)
    row_wide = lax.broadcasted_iota(jnp.int32, (BLOCK, n), 0)
    for k in range(n // BLOCK):
        rows = [work_ref[s, k * BLOCK : (k + 1) * BLOCK, :] for s in range(shifts)]
        near = (k * BLOCK) // LANES * LANES
        packed = jnp.zeros((BLOCK, LANES), jnp.float32)
        for s in range(shifts):
            move = (BLOCK * s - (k * BLOCK - near)) % LANES
            piece = rows[s][:, near : near + LANES]
            if move:
                piece = pltpu.roll(piece, move, axis=1)
            packed = jnp.where(lane_small // BLOCK == s, piece, packed)
        inverse = packed_inverse(packed, BLOCK)
        left = jnp.concatenate(
            [jnp.where(lane_small // BLOCK == s, -inverse, 0.0) for s in range(shifts)], axis=0
        )
        own = (lane_wide >= k * BLOCK) & (lane_wide < (k + 1) * BLOCK)
        minus_eye = jnp.where(lane_wide == row_wide + k * BLOCK, -1.0, 0.0)
        bars = [jnp.where(own, minus_eye, r) for r in rows]
        swept = jnp.dot(
            left,
            jnp.concatenate(bars, axis=0),
            precision=lax.Precision.HIGHEST,
            preferred_element_type=jnp.float32,
        )
        for s in range(shifts):
            z = swept[s * BLOCK : (s + 1) * BLOCK, :]
            y1, y2, y3 = split3(jnp.where(own, 0.0, z))
            r1, r2, r3 = split3(bars[s])
            update = lax.dot_general(
                jnp.concatenate([y1, y1, y2, y2, y1, y3], axis=0),
                jnp.concatenate([r1, r2, r1, r2, r3, r1], axis=0),
                (((0,), (0,)), ((), ())),
                preferred_element_type=jnp.float32,
            )
            own_all = (lane_id >= k * BLOCK) & (lane_id < (k + 1) * BLOCK)
            work_ref[s] = jnp.where(own_all, 0.0, work_ref[s]) - update
            work_ref[s, k * BLOCK : (k + 1) * BLOCK, :] = z
    root = jnp.where(diag, ROOT_CONST, 0.0)
    for s in range(shifts):
        root = root - ROOT_COEF[s] * work_ref[s]
    inner = jnp.sum(root * innovation, axis=1, keepdims=True)
    weights = jnp.sum(root * inner, axis=0, keepdims=True) * (1.0 / (ensemble - 1.0))
    mixing = root + weights
    for pair in range(per // 2):
        lanes = slice(pair * 2 * LANES, (pair + 1) * 2 * LANES)
        mixed = jnp.dot(
            mixing,
            dev_ref[:, lanes],
            precision=lax.Precision.HIGHEST,
            preferred_element_type=jnp.float32,
        ) + mean_ref[0:1, lanes]
        for part in range(SPLIT):
            for i in range(2):
                out_refs[part][pl.ds(2 * pair + i, half, stride=per), :] = mixed[
                    part * half : (part + 1) * half, i * LANES : (i + 1) * LANES
                ]


def advance_kernel(main_ref, low_ref, high_ref, *refs, members, per):
    out_ref, buf_ref = refs[-2:]
    blocks = per // 3
    stride = main_ref.shape[0] // 8
    first = pl.program_id(0) * members

    def one(i, slot):
        m = first + i
        for at, ref, count in ((6, low_ref, 2), (8, main_ref, 8), (16, high_ref, 2)):
            parts = [ref[pl.ds(m * per + j, count, stride=stride), :] for j in range(per)]
            parts += [(1.0 + parts[cb]) * parts[2 * blocks + cb] for cb in range(blocks)]
            for j, part in enumerate(parts):
                buf_ref[slot, j, at : at + count, :] = part

        def load(f, shift):
            return jnp.concatenate(
                [buf_ref[slot, f * blocks + cb, 8 + shift : 16 + shift, :] for cb in range(blocks)], axis=1
            )

        slopes = tendency(load)
        for f in range(3):
            out_ref[i, f] = load(f, 0) + TIME_STEP * slopes[f]

    def some(i, _):
        for r in range(UNROLL):
            one(i * UNROLL + r, r)
        return 0

    lax.fori_loop(0, members // UNROLL, some, 0)


VMEM = pl.BlockSpec(memory_space=pltpu.VMEM)


def f32(*shape):
    return jax.ShapeDtypeStruct(shape, jnp.float32)


def make_start(prior, deviations, split):
    members, fields, rows, width = deviations.shape
    step = 16
    flat = fields * rows * width // LANES // split
    return pl.pallas_call(
        start_kernel,
        grid=(members // step,),
        in_specs=[
            pl.BlockSpec((fields, rows, width), lambda i: (0, 0, 0)),
            pl.BlockSpec((step, fields, rows, width), lambda i: (i, 0, 0, 0)),
        ],
        out_specs=[pl.BlockSpec((step * flat, LANES), lambda i: (i, 0))] * split,
        out_shape=[f32(members * flat, LANES)] * split,
        name="start",
    )(prior, deviations)


def runge_kutta(rows, tiles, members, blocks):
    per = 3 * blocks
    return pl.pallas_call(
        functools.partial(runge_kutta_kernel, tiles=tiles, members=members, blocks=blocks),
        in_specs=[VMEM],
        out_specs=VMEM,
        out_shape=f32(*rows.shape),
        scratch_shapes=[
            pltpu.VMEM((4 * blocks, tiles * 8 + 16, LANES), jnp.float32),
            pltpu.VMEM((4 * blocks, tiles * 8 + 16, LANES), jnp.float32),
            pltpu.VMEM((3, tiles * 8, blocks * LANES), jnp.float32),
        ],
        name="runge_kutta",
    )(rows)


def gram_pieces(slabs, cell, value, var, ensemble, per):
    return pl.pallas_call(
        functools.partial(gram_kernel, split=len(slabs), ensemble=ensemble, per=per),
        in_specs=[VMEM] * (3 + len(slabs)),
        out_specs=[VMEM] * 3,
        out_shape=[f32(ensemble // 2 * PIECE, LANES), f32(ensemble, per * LANES), f32(8, per * LANES)],
        name="gram",
    )(*slabs, cell, value, var)


def piece_sum(pieces):
    return pl.pallas_call(
        piece_sum_kernel, in_specs=[VMEM], out_specs=VMEM, out_shape=f32(*pieces.shape), name="piece_sum"
    )(pieces)


def analyse(pieces, dev, mean, ensemble, per):
    return pl.pallas_call(
        functools.partial(root_kernel, ensemble=ensemble, per=per),
        in_specs=[VMEM] * 3,
        out_specs=[VMEM] * SPLIT,
        out_shape=[f32(ensemble // SPLIT * per, LANES)] * SPLIT,
        scratch_shapes=[pltpu.VMEM((len(SHIFT), ensemble, ensemble), jnp.float32)],
        name="analyse",
    )(pieces, dev, mean)


def advance(main, low, high, earlier, part, split, members, per):
    step = 8
    width = per // 3 * LANES
    return pl.pallas_call(
        functools.partial(advance_kernel, members=step, per=per),
        grid=(members // step,),
        in_specs=[VMEM] * 3 + [pl.BlockSpec(memory_space=pl.ANY)] * len(earlier),
        out_specs=pl.BlockSpec((step, None, 3, 8, width), lambda i: (i, part, 0, 0, 0)),
        out_shape=f32(members, split, 3, 8, width),
        scratch_shapes=[pltpu.VMEM((UNROLL, per // 3 * 4, 24, LANES), jnp.float32)],
        input_output_aliases={3: 0} if earlier else {},
        name="advance",
    )(main, low, high, *earlier)


def exchange(rows, axes, count):
    moved = lax.all_to_all(rows.reshape(count, -1), axes, 0, 0, tiled=True)
    return moved.reshape(rows.shape)


def per_device(prior_mean_fields, ensemble_deviations, obs_cell, obs_value, obs_var):
    runners, tiles = lax.axis_size("runner"), lax.axis_size("tile")
    members_dev, _, _, width = ensemble_deviations.shape
    blocks = width // LANES
    per = 3 * blocks
    ensemble = members_dev * runners
    whole = ("runner", "tile")
    split = members_dev // tiles
    devices = runners * tiles
    starts = make_start(prior_mean_fields, ensemble_deviations, split)
    grids = [exchange(part, "tile", tiles) for part in starts]
    slabs = [exchange(runge_kutta(part, tiles, 1, blocks), whole, devices) for part in grids]
    pieces, dev, mean = gram_pieces(
        slabs, obs_cell.reshape(-1, 1), obs_value.reshape(-1, 1), obs_var.reshape(-1, 1), ensemble, per
    )
    pieces = exchange(pieces, whole, devices)
    pieces = exchange(piece_sum(pieces), whole, devices)
    edge = 2 * tiles * per
    forward = [(i, (i + 1) % tiles) for i in range(tiles)]
    backward = [(target, source) for source, target in forward]
    analysed = [exchange(part, "runner", runners) for part in analyse(pieces, dev, mean, ensemble, per)]
    halos = [
        (lax.ppermute(part[-edge:], "tile", forward), lax.ppermute(part[:edge], "tile", backward))
        for part in analysed
    ]
    earlier = []
    for i, (part, halo) in enumerate(zip(analysed, halos)):
        earlier = [advance(part, *halo, earlier, i, split, tiles, per)]
    return earlier[0].reshape(ensemble_deviations.shape)


def solution(mesh):
    placed = (
        P(None, "tile", None),
        P("runner", None, "tile", None),
        P("tile", "runner", None),
        P("tile", "runner", None),
        P("tile", "runner", None),
    )
    return jax.shard_map(
        per_device,
        mesh=mesh,
        in_specs=placed,
        out_specs=P("runner", None, "tile", None),
        check_vma=False,
    )
```

```python
import functools
import math

import jax
import jax.numpy as jnp
from jax import lax
from jax.experimental import pallas as pl
from jax.experimental.pallas import tpu as pltpu
from jax.sharding import PartitionSpec as P

TIME_STEP = 0.25
CORIOLIS = 0.2
LANES = 128
ROOT2 = math.sqrt(2.0)
POLE_LOW = 3.0 - 2.0 * ROOT2
POLE_HIGH = 3.0 + 2.0 * ROOT2
SHIFT = (0.0, 1.0, POLE_LOW, POLE_HIGH)
ROOT_CONST = 0.125
ROOT_COEF = (
    0.125,
    0.5,
    2.0 * (1.0 - POLE_LOW) / (POLE_HIGH - POLE_LOW),
    2.0 * (POLE_HIGH - 1.0) / (POLE_HIGH - POLE_LOW),
)
BLOCK = 32
PANEL = 16
PIECE = 3


def start_kernel(prior_ref, dev_ref, out_ref):
    members, fields, rows, width = dev_ref.shape
    for m in range(members):
        for f in range(fields):
            for cb in range(width // LANES):
                at = ((m * fields + f) * (width // LANES) + cb) * rows
                lanes = slice(cb * LANES, (cb + 1) * LANES)
                out_ref[at : at + rows, :] = dev_ref[m, f, :, lanes] + prior_ref[f, :, lanes]


def roll_x(field, shift):
    return pltpu.roll(field, shift % field.shape[-1], axis=field.ndim - 1)


def along_x(field):
    return (roll_x(field, -1) - roll_x(field, 1)) - 0.125 * (roll_x(field, -2) - roll_x(field, 2))


def along_y(load, f):
    return (load(f, 1) - load(f, -1)) - 0.125 * (load(f, 2) - load(f, -2))


SLOPE = 8.0 / 12.0


def tendency(load):
    h, u, v = (load(f, 0) for f in range(3))
    height = -SLOPE * (along_x((1.0 + h) * u) + along_y(load, 3))
    east = CORIOLIS * v - SLOPE * (u * along_x(u) + v * along_y(load, 1) + along_x(h))
    north = -CORIOLIS * u - SLOPE * (u * along_x(v) + v * along_y(load, 2) + along_y(load, 0))
    return height, east, north


UNROLL = 4


def runge_kutta_kernel(in_ref, out_ref, even_ref, odd_ref, acc_ref, *, tiles, members, blocks):
    per = 3 * blocks
    grid_rows = tiles * 8
    sides = (even_ref, odd_ref)

    def split(value):
        return [value[:, cb * LANES : (cb + 1) * LANES] for cb in range(blocks)]

    def every_tile(step):
        def some(i, _):
            for r in range(UNROLL):
                step(i * UNROLL + r)
            return 0

        lax.fori_loop(0, tiles // UNROLL, some, 0)

    def member_step(m, _):
        def start_of(t, f):
            return jnp.concatenate(
                [in_ref[pl.ds(((t * members + m) * per + f * blocks + cb) * 8, 8), :] for cb in range(blocks)],
                axis=1,
            )

        def put(ref, t, values):
            flux = (1.0 + values[0]) * values[2]
            for f, value in enumerate((*values, flux)):
                for cb, part in enumerate(split(value)):
                    ref[f * blocks + cb, pl.ds(8 + t * 8, 8), :] = part

        def wrap(ref):
            for j in range(4 * blocks):
                ref[j, 0:8, :] = ref[j, grid_rows : grid_rows + 8, :]
                ref[j, grid_rows + 8 : grid_rows + 16, :] = ref[j, 8:16, :]

        every_tile(lambda t: put(even_ref, t, [start_of(t, f) for f in range(3)]))
        wrap(even_ref)
        for stage in range(4):
            here, there = sides[stage % 2], sides[1 - stage % 2]

            def step(t, stage=stage, here=here, there=there):
                def load(f, shift):
                    return jnp.concatenate(
                        [here[f * blocks + cb, pl.ds(8 + t * 8 + shift, 8), :] for cb in range(blocks)],
                        axis=1,
                    )

                slopes = tendency(load)
                rows = pl.ds(t * 8, 8)
                nexts = []
                for f in range(3):
                    start = start_of(t, f)
                    weight = TIME_STEP / 6.0 * (1.0 if stage in (0, 3) else 2.0)
                    total = (start if stage == 0 else acc_ref[f, rows, :]) + weight * slopes[f]
                    if stage < 3:
                        acc_ref[f, rows, :] = total
                        nexts.append(start + TIME_STEP * (1.0 if stage == 2 else 0.5) * slopes[f])
                    else:
                        for cb, part in enumerate(split(total)):
                            at = t * (members * per) + m * per + f * blocks + cb
                            out_ref[pl.ds(at, 8, stride=tiles * members * per), :] = part
                if stage < 3:
                    put(there, t, nexts)

            every_tile(step)
            if stage < 3:
                wrap(there)
        return 0

    lax.fori_loop(0, members, member_step, 0)


def gram_kernel(
    in_ref, cell_ref, value_ref, var_ref, pack_ref, dev_ref, mean_ref, buf_ref, sem_ref, *, ensemble, per
):
    inverse = 1.0 / var_ref[...]
    count = inverse.shape[1]
    observed = jnp.concatenate(
        [cell_ref[...].astype(jnp.float32), inverse, value_ref[...] * inverse, jnp.zeros((5, count), jnp.float32)],
        axis=0,
    ).T
    cells, inv_var, val_w = (
        jnp.broadcast_to(observed[:, i : i + 1], (count, LANES)) for i in range(3)
    )
    cells = cells.astype(jnp.int32)
    copies = []
    lane = lax.broadcasted_iota(jnp.int32, (count, LANES), 1)
    total = jnp.zeros((ensemble + 8, ensemble), jnp.float32)
    for pair in range(per // 2):
        devs, lefts = [], []
        for j in (2 * pair, 2 * pair + 1):
            hit = cells == lane + j * LANES
            w = jnp.sum(jnp.where(hit, inv_var, 0.0), axis=0, keepdims=True)
            vw = jnp.sum(jnp.where(hit, val_w, 0.0), axis=0, keepdims=True)
            full = in_ref[pl.ds(j, ensemble, stride=per), :]
            mean = jnp.sum(full, axis=0, keepdims=True) * (1.0 / ensemble)
            dev = full - mean
            buf_ref[:, j * LANES : (j + 1) * LANES] = dev
            mean_ref[:, j * LANES : (j + 1) * LANES] = jnp.broadcast_to(mean, (8, LANES))
            devs.append(dev)
            z = jnp.broadcast_to(vw - mean * w, (8, LANES))
            lefts.append(jnp.concatenate([dev * w, z], axis=0))
        lanes = slice(pair * 2 * LANES, (pair + 1) * 2 * LANES)
        copies.append(pltpu.make_async_copy(buf_ref.at[:, lanes], dev_ref.at[:, lanes], sem_ref.at[pair]))
        copies[-1].start()
        total = total + lax.dot_general(
            jnp.concatenate(lefts, axis=1),
            jnp.concatenate(devs, axis=1),
            (((1,), (1,)), ((), ())),
            precision=lax.Precision.HIGHEST,
            preferred_element_type=jnp.float32,
        )
    half = ensemble // 2
    sub = lax.broadcasted_iota(jnp.int32, (half, LANES), 0)
    col = lax.broadcasted_iota(jnp.int32, (half, LANES), 1)
    low, high = total[half:ensemble, LANES:], total[:half, :LANES]
    diagonal = jnp.sum(jnp.where(sub == col, low, 0.0), axis=0, keepdims=True)
    inn = total[ensemble : ensemble + 1, :]
    pack_ref[pl.ds(0, half, stride=PIECE), :] = total[:half, LANES:]
    pack_ref[pl.ds(1, half, stride=PIECE), :] = jnp.where(col >= sub, high, low)
    extra = jnp.zeros((half, LANES), jnp.float32)
    for i, row in enumerate((inn[:, :LANES], inn[:, LANES:], diagonal)):
        extra = jnp.where(sub == i, jnp.broadcast_to(row, (half, LANES)), extra)
    pack_ref[pl.ds(2, half, stride=PIECE), :] = extra
    for copy in copies:
        copy.wait()


def unpack_gram(ref, half):
    sub = lax.broadcasted_iota(jnp.int32, (half, LANES), 0)
    col = lax.broadcasted_iota(jnp.int32, (half, LANES), 1)
    cross = ref[pl.ds(0, half, stride=PIECE), :]
    both = ref[pl.ds(1, half, stride=PIECE), :]
    turned = both.T
    first = jnp.where(col >= sub, both, turned)
    second = jnp.where(col < sub, both, turned)
    second = jnp.where(col == sub, jnp.broadcast_to(ref[2 * PIECE + 2 : 2 * PIECE + 3, :], (half, LANES)), second)
    gram = jnp.concatenate(
        [jnp.concatenate([first, cross], axis=1), jnp.concatenate([cross.T, second], axis=1)], axis=0
    )
    innovation = jnp.concatenate([ref[2:3, :], ref[PIECE + 2 : PIECE + 3, :]], axis=1)
    return gram, innovation


def piece_sum_kernel(in_ref, out_ref):
    count = in_ref.shape[0] // PIECE
    for q in range(PIECE):
        total = jnp.sum(in_ref[pl.ds(q, count, stride=PIECE), :], axis=0, keepdims=True)
        out_ref[pl.ds(q, count, stride=PIECE), :] = jnp.broadcast_to(total, (count, LANES))


def split3(x):
    hi = x.astype(jnp.bfloat16)
    rest = x - hi.astype(jnp.float32)
    mid = rest.astype(jnp.bfloat16)
    low = (rest - mid.astype(jnp.float32)).astype(jnp.bfloat16)
    return hi, mid, low


def packed_inverse(packed, group):
    shape = (8, LANES)
    lane = lax.broadcasted_iota(jnp.int32, shape, 1)
    sub = lax.broadcasted_iota(jnp.int32, shape, 0)
    within = lane % group
    first = lane - within
    count = group // 8
    rows = [packed[8 * i : 8 * i + 8, :] for i in range(count)]

    def spread(parts, k):
        return jnp.broadcast_to(parts[k // 8][k % 8 : k % 8 + 1, :], shape)

    def sweep(parts, column, k, row):
        out = [part - c * row for part, c in zip(parts, column)]
        out[k // 8] = jnp.where(sub == k % 8, row, out[k // 8])
        return out

    for k0 in range(0, group, PANEL):
        panel = range(k0, k0 + PANEL)
        columns = {k: [jnp.take_along_axis(part, first + k, axis=1) for part in rows] for k in panel}
        for k in panel:
            column = columns.pop(k)
            inv = 1.0 / spread(column, k)
            for j in columns:
                columns[j] = sweep(columns[j], column, k, spread(columns[j], k) * inv)
            row = jnp.where(within == k, -1.0, spread(rows, k)) * inv
            rows = sweep([jnp.where(within == k, 0.0, part) for part in rows], column, k, row)
    return jnp.concatenate(rows, axis=0)


def root_kernel(in_ref, dev_ref, mean_ref, out_ref, work_ref, buf_ref, sem_ref, *, ensemble, per):
    fetch = pltpu.make_async_copy(dev_ref, buf_ref, sem_ref)
    fetch.start()
    half = ensemble // 2
    n = ensemble
    row_id = lax.broadcasted_iota(jnp.int32, (n, n), 0)
    lane_id = lax.broadcasted_iota(jnp.int32, (n, n), 1)
    diag = row_id == lane_id
    gram, innovation = unpack_gram(in_ref, half)
    matrix = gram * (1.0 / (ensemble - 1.0))
    for s, shift in enumerate(SHIFT):
        work_ref[s] = matrix + jnp.where(diag, 1.0 + shift, 0.0)
    shifts = len(SHIFT)
    lane_small = lax.broadcasted_iota(jnp.int32, (BLOCK, LANES), 1)
    lane_wide = lax.broadcasted_iota(jnp.int32, (BLOCK, n), 1)
    row_wide = lax.broadcasted_iota(jnp.int32, (BLOCK, n), 0)
    for k in range(n // BLOCK):
        rows = [work_ref[s, k * BLOCK : (k + 1) * BLOCK, :] for s in range(shifts)]
        near = (k * BLOCK) // LANES * LANES
        packed = jnp.zeros((BLOCK, LANES), jnp.float32)
        for s in range(shifts):
            move = (BLOCK * s - (k * BLOCK - near)) % LANES
            piece = rows[s][:, near : near + LANES]
            if move:
                piece = pltpu.roll(piece, move, axis=1)
            packed = jnp.where(lane_small // BLOCK == s, piece, packed)
        inverse = packed_inverse(packed, BLOCK)
        left = jnp.concatenate(
            [jnp.where(lane_small // BLOCK == s, -inverse, 0.0) for s in range(shifts)], axis=0
        )
        own = (lane_wide >= k * BLOCK) & (lane_wide < (k + 1) * BLOCK)
        minus_eye = jnp.where(lane_wide == row_wide + k * BLOCK, -1.0, 0.0)
        bars = [jnp.where(own, minus_eye, r) for r in rows]
        swept = jnp.dot(
            left,
            jnp.concatenate(bars, axis=0),
            precision=lax.Precision.HIGHEST,
            preferred_element_type=jnp.float32,
        )
        for s in range(shifts):
            z = swept[s * BLOCK : (s + 1) * BLOCK, :]
            y1, y2, y3 = split3(jnp.where(own, 0.0, z))
            r1, r2, r3 = split3(bars[s])
            update = lax.dot_general(
                jnp.concatenate([y1, y1, y2, y2, y1, y3], axis=0),
                jnp.concatenate([r1, r2, r1, r2, r3, r1], axis=0),
                (((0,), (0,)), ((), ())),
                preferred_element_type=jnp.float32,
            )
            own_all = (lane_id >= k * BLOCK) & (lane_id < (k + 1) * BLOCK)
            work_ref[s] = jnp.where(own_all, 0.0, work_ref[s]) - update
            work_ref[s, k * BLOCK : (k + 1) * BLOCK, :] = z
    root = jnp.where(diag, ROOT_CONST, 0.0)
    for s in range(shifts):
        root = root - ROOT_COEF[s] * work_ref[s]
    inner = jnp.sum(root * innovation, axis=1, keepdims=True)
    weights = jnp.sum(root * inner, axis=0, keepdims=True) * (1.0 / (ensemble - 1.0))
    mixing = root + weights
    fetch.wait()
    for pair in range(per // 2):
        lanes = slice(pair * 2 * LANES, (pair + 1) * 2 * LANES)
        mixed = jnp.dot(
            mixing,
            buf_ref[:, lanes],
            precision=lax.Precision.HIGHEST,
            preferred_element_type=jnp.float32,
        ) + mean_ref[0:1, lanes]
        for i in range(2):
            out_ref[pl.ds(2 * pair + i, ensemble, stride=per), :] = mixed[:, i * LANES : (i + 1) * LANES]


def advance_kernel(main_ref, low_ref, high_ref, out_ref, buf_ref, *, members, per):
    blocks = per // 3
    here = main_ref.reshape(8 * members * per, LANES)
    stride = low_ref.shape[0] // 2
    first = pl.program_id(0) * members

    def one(i, slot):
        m = first + i
        for at, ref, count, row, apart in (
            (6, low_ref, 2, m * per, stride),
            (8, here, 8, i * per, members * per),
            (16, high_ref, 2, m * per, stride),
        ):
            parts = [ref[pl.ds(row + j, count, stride=apart), :] for j in range(per)]
            parts += [(1.0 + parts[cb]) * parts[2 * blocks + cb] for cb in range(blocks)]
            for j, part in enumerate(parts):
                buf_ref[slot, j, at : at + count, :] = part

        def load(f, shift):
            return jnp.concatenate(
                [buf_ref[slot, f * blocks + cb, 8 + shift : 16 + shift, :] for cb in range(blocks)], axis=1
            )

        slopes = tendency(load)
        for f in range(3):
            out_ref[i, f] = load(f, 0) + TIME_STEP * slopes[f]

    def some(i, _):
        for r in range(UNROLL):
            one(i * UNROLL + r, r)
        return 0

    lax.fori_loop(0, members // UNROLL, some, 0)


VMEM = pl.BlockSpec(memory_space=pltpu.VMEM)
HBM = pl.BlockSpec(memory_space=pl.ANY)


def f32(*shape):
    return jax.ShapeDtypeStruct(shape, jnp.float32)


def near(*shape):
    return pltpu.VMEM(shape, jnp.float32)


def in_vmem(x):
    return pltpu.with_memory_space_constraint(x, pltpu.VMEM)


def make_start(prior, deviations):
    members, fields, rows, width = deviations.shape
    step = 16
    return pl.pallas_call(
        start_kernel,
        grid=(members // step,),
        in_specs=[
            pl.BlockSpec((fields, rows, width), lambda i: (0, 0, 0)),
            pl.BlockSpec((step, fields, rows, width), lambda i: (i, 0, 0, 0)),
        ],
        out_specs=pl.BlockSpec((step * fields * rows * width // LANES, LANES), lambda i: (i, 0)),
        out_shape=near(members * fields * rows * width // LANES, LANES),
        name="start",
    )(prior, deviations)


def runge_kutta(rows, tiles, members, blocks):
    per = 3 * blocks
    return pl.pallas_call(
        functools.partial(runge_kutta_kernel, tiles=tiles, members=members, blocks=blocks),
        in_specs=[VMEM],
        out_specs=VMEM,
        out_shape=near(*rows.shape),
        scratch_shapes=[
            pltpu.VMEM((4 * blocks, tiles * 8 + 16, LANES), jnp.float32),
            pltpu.VMEM((4 * blocks, tiles * 8 + 16, LANES), jnp.float32),
            pltpu.VMEM((3, tiles * 8, blocks * LANES), jnp.float32),
        ],
        name="runge_kutta",
    )(in_vmem(rows))


def gram_pieces(rows, cell, value, var, ensemble, per):
    return pl.pallas_call(
        functools.partial(gram_kernel, ensemble=ensemble, per=per),
        in_specs=[VMEM] * 4,
        out_specs=[VMEM, HBM, VMEM],
        out_shape=[near(ensemble // 2 * PIECE, LANES), f32(ensemble, per * LANES), near(8, per * LANES)],
        scratch_shapes=[
            pltpu.VMEM((ensemble, per * LANES), jnp.float32),
            pltpu.SemaphoreType.DMA((per // 2,)),
        ],
        name="gram",
    )(in_vmem(rows), cell, value, var)


def piece_sum(pieces):
    return pl.pallas_call(
        piece_sum_kernel, in_specs=[VMEM], out_specs=VMEM, out_shape=near(*pieces.shape), name="piece_sum"
    )(in_vmem(pieces))


def analyse(pieces, dev, mean, ensemble, per):
    return pl.pallas_call(
        functools.partial(root_kernel, ensemble=ensemble, per=per),
        in_specs=[VMEM, HBM, VMEM],
        out_specs=VMEM,
        out_shape=near(ensemble * per, LANES),
        scratch_shapes=[
            pltpu.VMEM((len(SHIFT), ensemble, ensemble), jnp.float32),
            pltpu.VMEM((ensemble, per * LANES), jnp.float32),
            pltpu.SemaphoreType.DMA(()),
        ],
        name="analyse",
    )(in_vmem(pieces), dev, in_vmem(mean))


def advance(main, low, high, members, per):
    step = 8
    return pl.pallas_call(
        functools.partial(advance_kernel, members=step, per=per),
        grid=(members // step,),
        in_specs=[pl.BlockSpec((8, step * per, LANES), lambda i: (0, i, 0)), VMEM, VMEM],
        out_specs=pl.BlockSpec((step, 3, 8, per // 3 * LANES), lambda i: (i, 0, 0, 0)),
        out_shape=f32(members, 3, 8, per // 3 * LANES),
        scratch_shapes=[pltpu.VMEM((UNROLL, per // 3 * 4, 24, LANES), jnp.float32)],
        name="advance",
    )(main.reshape(8, members * per, LANES), in_vmem(low), in_vmem(high))


def exchange(rows, axes, count):
    moved = lax.all_to_all(rows.reshape(count, -1), axes, 0, 0, tiled=True)
    return moved.reshape(rows.shape)


def per_device(prior_mean_fields, ensemble_deviations, obs_cell, obs_value, obs_var):
    runners, tiles = lax.axis_size("runner"), lax.axis_size("tile")
    members_dev, _, _, width = ensemble_deviations.shape
    blocks = width // LANES
    per = 3 * blocks
    ensemble = members_dev * runners
    whole = ("runner", "tile")
    start = make_start(prior_mean_fields, ensemble_deviations)
    grids = exchange(start, "tile", tiles)
    forecast = runge_kutta(grids, tiles, members_dev // tiles, blocks)
    slab = exchange(forecast, whole, runners * tiles)
    pieces, dev, mean = gram_pieces(
        slab, obs_cell[0], obs_value[0], obs_var[0], ensemble, per
    )
    pieces = exchange(pieces, whole, runners * tiles)
    pieces = exchange(piece_sum(pieces), whole, runners * tiles)
    analysed = exchange(analyse(pieces, dev, mean, ensemble, per), "runner", runners)
    edge = 2 * members_dev * per
    forward = [(i, (i + 1) % tiles) for i in range(tiles)]
    backward = [(target, source) for source, target in forward]
    low = lax.ppermute(analysed[-edge:], "tile", forward)
    high = lax.ppermute(analysed[:edge], "tile", backward)
    return advance(analysed, low, high, members_dev, per)


def solution(mesh):
    placed = (
        P(None, "tile", None),
        P("runner", None, "tile", None),
        P("tile", "runner", None),
        P("tile", "runner", None),
        P("tile", "runner", None),
    )
    return jax.shard_map(
        per_device,
        mesh=mesh,
        in_specs=placed,
        out_specs=P("runner", None, "tile", None),
        check_vma=False,
    )
```

```python
import functools
import math

import jax
import jax.numpy as jnp
from jax import lax
from jax.experimental import pallas as pl
from jax.experimental.pallas import tpu as pltpu
from jax.sharding import PartitionSpec as P

TIME_STEP = 0.25
CORIOLIS = 0.2
LANES = 128
ROOT2 = math.sqrt(2.0)
POLE_LOW = 3.0 - 2.0 * ROOT2
POLE_HIGH = 3.0 + 2.0 * ROOT2
SHIFT = (0.0, 1.0, POLE_LOW, POLE_HIGH)
ROOT_CONST = 0.125
ROOT_COEF = (
    0.125,
    0.5,
    2.0 * (1.0 - POLE_LOW) / (POLE_HIGH - POLE_LOW),
    2.0 * (POLE_HIGH - 1.0) / (POLE_HIGH - POLE_LOW),
)
BLOCK = 32
PANEL = 16
PIECE = 3


def start_kernel(prior_ref, dev_ref, out_ref):
    members, fields, rows, width = dev_ref.shape
    for m in range(members):
        for f in range(fields):
            for cb in range(width // LANES):
                at = ((m * fields + f) * (width // LANES) + cb) * rows
                lanes = slice(cb * LANES, (cb + 1) * LANES)
                out_ref[at : at + rows, :] = dev_ref[m, f, :, lanes] + prior_ref[f, :, lanes]


def roll_x(field, shift):
    return pltpu.roll(field, shift % field.shape[-1], axis=field.ndim - 1)


def along_x(field):
    return (roll_x(field, -1) - roll_x(field, 1)) - 0.125 * (roll_x(field, -2) - roll_x(field, 2))


def along_y(load, f):
    return (load(f, 1) - load(f, -1)) - 0.125 * (load(f, 2) - load(f, -2))


SLOPE = 8.0 / 12.0


def tendency(load):
    h, u, v = (load(f, 0) for f in range(3))
    height = -SLOPE * (along_x((1.0 + h) * u) + along_y(load, 3))
    east = CORIOLIS * v - SLOPE * (u * along_x(u) + v * along_y(load, 1) + along_x(h))
    north = -CORIOLIS * u - SLOPE * (u * along_x(v) + v * along_y(load, 2) + along_y(load, 0))
    return height, east, north


UNROLL = 4


def runge_kutta_kernel(in_ref, out_ref, even_ref, odd_ref, acc_ref, *, tiles, members, blocks):
    per = 3 * blocks
    grid_rows = tiles * 8
    sides = (even_ref, odd_ref)

    def split(value):
        return [value[:, cb * LANES : (cb + 1) * LANES] for cb in range(blocks)]

    def every_tile(step):
        def some(i, _):
            for r in range(UNROLL):
                step(i * UNROLL + r)
            return 0

        lax.fori_loop(0, tiles // UNROLL, some, 0)

    def member_step(m, _):
        def start_of(t, f):
            return jnp.concatenate(
                [in_ref[pl.ds(((t * members + m) * per + f * blocks + cb) * 8, 8), :] for cb in range(blocks)],
                axis=1,
            )

        def put(ref, t, values):
            flux = (1.0 + values[0]) * values[2]
            for f, value in enumerate((*values, flux)):
                for cb, part in enumerate(split(value)):
                    ref[f * blocks + cb, pl.ds(8 + t * 8, 8), :] = part

        def wrap(ref):
            for j in range(4 * blocks):
                ref[j, 0:8, :] = ref[j, grid_rows : grid_rows + 8, :]
                ref[j, grid_rows + 8 : grid_rows + 16, :] = ref[j, 8:16, :]

        every_tile(lambda t: put(even_ref, t, [start_of(t, f) for f in range(3)]))
        wrap(even_ref)
        for stage in range(4):
            here, there = sides[stage % 2], sides[1 - stage % 2]

            def step(t, stage=stage, here=here, there=there):
                def load(f, shift):
                    return jnp.concatenate(
                        [here[f * blocks + cb, pl.ds(8 + t * 8 + shift, 8), :] for cb in range(blocks)],
                        axis=1,
                    )

                slopes = tendency(load)
                rows = pl.ds(t * 8, 8)
                nexts = []
                for f in range(3):
                    start = start_of(t, f)
                    weight = TIME_STEP / 6.0 * (1.0 if stage in (0, 3) else 2.0)
                    total = (start if stage == 0 else acc_ref[f, rows, :]) + weight * slopes[f]
                    if stage < 3:
                        acc_ref[f, rows, :] = total
                        nexts.append(start + TIME_STEP * (1.0 if stage == 2 else 0.5) * slopes[f])
                    else:
                        for cb, part in enumerate(split(total)):
                            at = t * (members * per) + m * per + f * blocks + cb
                            out_ref[pl.ds(at, 8, stride=tiles * members * per), :] = part
                if stage < 3:
                    put(there, t, nexts)

            every_tile(step)
            if stage < 3:
                wrap(there)
        return 0

    lax.fori_loop(0, members, member_step, 0)


def gram_kernel(
    in_ref, cell_ref, value_ref, var_ref, pack_ref, dev_ref, mean_ref, buf_ref, sem_ref, *, ensemble, per
):
    inverse = 1.0 / var_ref[...]
    count = inverse.shape[1]
    observed = jnp.concatenate(
        [cell_ref[...].astype(jnp.float32), inverse, value_ref[...] * inverse, jnp.zeros((5, count), jnp.float32)],
        axis=0,
    ).T
    cells, inv_var, val_w = (
        jnp.broadcast_to(observed[:, i : i + 1], (count, LANES)) for i in range(3)
    )
    cells = cells.astype(jnp.int32)
    copies = []
    lane = lax.broadcasted_iota(jnp.int32, (count, LANES), 1)
    total = jnp.zeros((ensemble + 8, ensemble), jnp.float32)
    for pair in range(per // 2):
        devs, lefts = [], []
        for j in (2 * pair, 2 * pair + 1):
            hit = cells == lane + j * LANES
            w = jnp.sum(jnp.where(hit, inv_var, 0.0), axis=0, keepdims=True)
            vw = jnp.sum(jnp.where(hit, val_w, 0.0), axis=0, keepdims=True)
            full = in_ref[pl.ds(j, ensemble, stride=per), :]
            mean = jnp.sum(full, axis=0, keepdims=True) * (1.0 / ensemble)
            dev = full - mean
            buf_ref[:, j * LANES : (j + 1) * LANES] = dev
            mean_ref[:, j * LANES : (j + 1) * LANES] = jnp.broadcast_to(mean, (8, LANES))
            devs.append(dev)
            z = jnp.broadcast_to(vw - mean * w, (8, LANES))
            lefts.append(jnp.concatenate([dev * w, z], axis=0))
        lanes = slice(pair * 2 * LANES, (pair + 1) * 2 * LANES)
        copies.append(pltpu.make_async_copy(buf_ref.at[:, lanes], dev_ref.at[:, lanes], sem_ref.at[pair]))
        copies[-1].start()
        total = total + lax.dot_general(
            jnp.concatenate(lefts, axis=1),
            jnp.concatenate(devs, axis=1),
            (((1,), (1,)), ((), ())),
            precision=lax.Precision.HIGHEST,
            preferred_element_type=jnp.float32,
        )
    half = ensemble // 2
    sub = lax.broadcasted_iota(jnp.int32, (half, LANES), 0)
    col = lax.broadcasted_iota(jnp.int32, (half, LANES), 1)
    low, high = total[half:ensemble, LANES:], total[:half, :LANES]
    diagonal = jnp.sum(jnp.where(sub == col, low, 0.0), axis=0, keepdims=True)
    inn = total[ensemble : ensemble + 1, :]
    pack_ref[pl.ds(0, half, stride=PIECE), :] = total[:half, LANES:]
    pack_ref[pl.ds(1, half, stride=PIECE), :] = jnp.where(col >= sub, high, low)
    extra = jnp.zeros((half, LANES), jnp.float32)
    for i, row in enumerate((inn[:, :LANES], inn[:, LANES:], diagonal)):
        extra = jnp.where(sub == i, jnp.broadcast_to(row, (half, LANES)), extra)
    pack_ref[pl.ds(2, half, stride=PIECE), :] = extra
    for copy in copies:
        copy.wait()


def unpack_gram(ref, half):
    sub = lax.broadcasted_iota(jnp.int32, (half, LANES), 0)
    col = lax.broadcasted_iota(jnp.int32, (half, LANES), 1)
    cross = ref[pl.ds(0, half, stride=PIECE), :]
    both = ref[pl.ds(1, half, stride=PIECE), :]
    turned = both.T
    first = jnp.where(col >= sub, both, turned)
    second = jnp.where(col < sub, both, turned)
    second = jnp.where(col == sub, jnp.broadcast_to(ref[2 * PIECE + 2 : 2 * PIECE + 3, :], (half, LANES)), second)
    gram = jnp.concatenate(
        [jnp.concatenate([first, cross], axis=1), jnp.concatenate([cross.T, second], axis=1)], axis=0
    )
    innovation = jnp.concatenate([ref[2:3, :], ref[PIECE + 2 : PIECE + 3, :]], axis=1)
    return gram, innovation


def piece_sum_kernel(in_ref, out_ref):
    count = in_ref.shape[0] // PIECE
    for q in range(PIECE):
        total = jnp.sum(in_ref[pl.ds(q, count, stride=PIECE), :], axis=0, keepdims=True)
        out_ref[pl.ds(q, count, stride=PIECE), :] = jnp.broadcast_to(total, (count, LANES))


def split3(x):
    hi = x.astype(jnp.bfloat16)
    rest = x - hi.astype(jnp.float32)
    mid = rest.astype(jnp.bfloat16)
    low = (rest - mid.astype(jnp.float32)).astype(jnp.bfloat16)
    return hi, mid, low


def packed_inverse(packed, group):
    shape = (8, LANES)
    lane = lax.broadcasted_iota(jnp.int32, shape, 1)
    sub = lax.broadcasted_iota(jnp.int32, shape, 0)
    within = lane % group
    first = lane - within
    count = group // 8
    rows = [packed[8 * i : 8 * i + 8, :] for i in range(count)]

    def spread(parts, k):
        return jnp.broadcast_to(parts[k // 8][k % 8 : k % 8 + 1, :], shape)

    def sweep(parts, column, k, row):
        out = [part - c * row for part, c in zip(parts, column)]
        out[k // 8] = jnp.where(sub == k % 8, row, out[k // 8])
        return out

    for k0 in range(0, group, PANEL):
        panel = range(k0, k0 + PANEL)
        columns = {k: [jnp.take_along_axis(part, first + k, axis=1) for part in rows] for k in panel}
        for k in panel:
            column = columns.pop(k)
            inv = 1.0 / spread(column, k)
            for j in columns:
                columns[j] = sweep(columns[j], column, k, spread(columns[j], k) * inv)
            row = jnp.where(within == k, -1.0, spread(rows, k)) * inv
            rows = sweep([jnp.where(within == k, 0.0, part) for part in rows], column, k, row)
    return jnp.concatenate(rows, axis=0)


def root_kernel(in_ref, dev_ref, mean_ref, out_ref, work_ref, buf_ref, sem_ref, *, ensemble, per):
    fetch = pltpu.make_async_copy(dev_ref, buf_ref, sem_ref)
    fetch.start()
    half = ensemble // 2
    n = ensemble
    row_id = lax.broadcasted_iota(jnp.int32, (n, n), 0)
    lane_id = lax.broadcasted_iota(jnp.int32, (n, n), 1)
    diag = row_id == lane_id
    gram, innovation = unpack_gram(in_ref, half)
    matrix = gram * (1.0 / (ensemble - 1.0))
    for s, shift in enumerate(SHIFT):
        work_ref[s] = matrix + jnp.where(diag, 1.0 + shift, 0.0)
    shifts = len(SHIFT)
    lane_small = lax.broadcasted_iota(jnp.int32, (BLOCK, LANES), 1)
    lane_wide = lax.broadcasted_iota(jnp.int32, (BLOCK, n), 1)
    row_wide = lax.broadcasted_iota(jnp.int32, (BLOCK, n), 0)
    for k in range(n // BLOCK):
        rows = [work_ref[s, k * BLOCK : (k + 1) * BLOCK, :] for s in range(shifts)]
        near = (k * BLOCK) // LANES * LANES
        packed = jnp.zeros((BLOCK, LANES), jnp.float32)
        for s in range(shifts):
            move = (BLOCK * s - (k * BLOCK - near)) % LANES
            piece = rows[s][:, near : near + LANES]
            if move:
                piece = pltpu.roll(piece, move, axis=1)
            packed = jnp.where(lane_small // BLOCK == s, piece, packed)
        inverse = packed_inverse(packed, BLOCK)
        left = jnp.concatenate(
            [jnp.where(lane_small // BLOCK == s, -inverse, 0.0) for s in range(shifts)], axis=0
        )
        own = (lane_wide >= k * BLOCK) & (lane_wide < (k + 1) * BLOCK)
        minus_eye = jnp.where(lane_wide == row_wide + k * BLOCK, -1.0, 0.0)
        bars = [jnp.where(own, minus_eye, r) for r in rows]
        swept = jnp.dot(
            left,
            jnp.concatenate(bars, axis=0),
            precision=lax.Precision.HIGHEST,
            preferred_element_type=jnp.float32,
        )
        for s in range(shifts):
            z = swept[s * BLOCK : (s + 1) * BLOCK, :]
            y1, y2, y3 = split3(jnp.where(own, 0.0, z))
            r1, r2, r3 = split3(bars[s])
            update = lax.dot_general(
                jnp.concatenate([y1, y1, y2, y2, y1, y3], axis=0),
                jnp.concatenate([r1, r2, r1, r2, r3, r1], axis=0),
                (((0,), (0,)), ((), ())),
                preferred_element_type=jnp.float32,
            )
            own_all = (lane_id >= k * BLOCK) & (lane_id < (k + 1) * BLOCK)
            work_ref[s] = jnp.where(own_all, 0.0, work_ref[s]) - update
            work_ref[s, k * BLOCK : (k + 1) * BLOCK, :] = z
    root = jnp.where(diag, ROOT_CONST, 0.0)
    for s in range(shifts):
        root = root - ROOT_COEF[s] * work_ref[s]
    inner = jnp.sum(root * innovation, axis=1, keepdims=True)
    weights = jnp.sum(root * inner, axis=0, keepdims=True) * (1.0 / (ensemble - 1.0))
    mixing = root + weights
    fetch.wait()
    for pair in range(per // 2):
        lanes = slice(pair * 2 * LANES, (pair + 1) * 2 * LANES)
        mixed = jnp.dot(
            mixing,
            buf_ref[:, lanes],
            precision=lax.Precision.HIGHEST,
            preferred_element_type=jnp.float32,
        ) + mean_ref[0:1, lanes]
        for i in range(2):
            out_ref[pl.ds(2 * pair + i, ensemble, stride=per), :] = mixed[:, i * LANES : (i + 1) * LANES]


def each_member(one, members):
    def some(i, _):
        for r in range(UNROLL):
            one(i * UNROLL + r, r)
        return 0

    lax.fori_loop(0, members // UNROLL, some, 0)


def clear(buf_ref):
    @pl.when(pl.program_id(0) == 0)
    def _():
        buf_ref[...] = jnp.zeros(buf_ref.shape, jnp.float32)


def with_flux(parts, blocks):
    return parts + [(1.0 + parts[cb]) * parts[2 * blocks + cb] for cb in range(blocks)]


def loader(buf_ref, slot, blocks):
    def load(f, shift):
        return jnp.concatenate(
            [buf_ref[slot, f * blocks + cb, 8 + shift : 16 + shift, :] for cb in range(blocks)], axis=1
        )

    return load


def advance_kernel(main_ref, out_ref, buf_ref, *, members, per):
    blocks = per // 3
    stride = main_ref.shape[0] // 8
    first = pl.program_id(0) * members
    clear(buf_ref)

    def one(i, slot):
        parts = [main_ref[pl.ds((first + i) * per + j, 8, stride=stride), :] for j in range(per)]
        for j, part in enumerate(with_flux(parts, blocks)):
            buf_ref[slot, j, 8:16, :] = part
        load = loader(buf_ref, slot, blocks)
        slopes = tendency(load)
        for f in range(3):
            out_ref[i, f] = load(f, 0) + TIME_STEP * slopes[f]

    each_member(one, members)


def border_kernel(main_ref, low_ref, high_ref, part_ref, out_ref, buf_ref, *, members, per):
    blocks = per // 3
    here = main_ref.reshape(8 * members * per, LANES)
    stride = low_ref.shape[0] // 2
    first = pl.program_id(0) * members
    clear(buf_ref)

    def one(i, slot):
        at = (first + i) * per
        for row, ref in ((6, low_ref), (16, high_ref)):
            parts = [ref[pl.ds(at + j, 2, stride=stride), :] for j in range(per)]
            for j, part in enumerate(with_flux(parts, blocks)):
                buf_ref[slot, j, row : row + 2, :] = part
        v = jnp.concatenate(
            [here[pl.ds(i * per + 2 * blocks + cb, 8, stride=members * per), :] for cb in range(blocks)], axis=1
        )
        load = loader(buf_ref, slot, blocks)
        rates = along_y(load, 3), v * along_y(load, 1), v * along_y(load, 2) + along_y(load, 0)
        for f in range(3):
            out_ref[i, f] = part_ref[i, f] - (TIME_STEP * SLOPE) * rates[f]

    each_member(one, members)


VMEM = pl.BlockSpec(memory_space=pltpu.VMEM)
HBM = pl.BlockSpec(memory_space=pl.ANY)


def f32(*shape):
    return jax.ShapeDtypeStruct(shape, jnp.float32)


def near(*shape):
    return pltpu.VMEM(shape, jnp.float32)


def in_vmem(x):
    return pltpu.with_memory_space_constraint(x, pltpu.VMEM)


def make_start(prior, deviations):
    members, fields, rows, width = deviations.shape
    step = 16
    return pl.pallas_call(
        start_kernel,
        grid=(members // step,),
        in_specs=[
            pl.BlockSpec((fields, rows, width), lambda i: (0, 0, 0)),
            pl.BlockSpec((step, fields, rows, width), lambda i: (i, 0, 0, 0)),
        ],
        out_specs=pl.BlockSpec((step * fields * rows * width // LANES, LANES), lambda i: (i, 0)),
        out_shape=near(members * fields * rows * width // LANES, LANES),
        name="start",
    )(prior, deviations)


def runge_kutta(rows, tiles, members, blocks):
    per = 3 * blocks
    return pl.pallas_call(
        functools.partial(runge_kutta_kernel, tiles=tiles, members=members, blocks=blocks),
        in_specs=[VMEM],
        out_specs=VMEM,
        out_shape=near(*rows.shape),
        scratch_shapes=[
            pltpu.VMEM((4 * blocks, tiles * 8 + 16, LANES), jnp.float32),
            pltpu.VMEM((4 * blocks, tiles * 8 + 16, LANES), jnp.float32),
            pltpu.VMEM((3, tiles * 8, blocks * LANES), jnp.float32),
        ],
        name="runge_kutta",
    )(in_vmem(rows))


def gram_pieces(rows, cell, value, var, ensemble, per):
    return pl.pallas_call(
        functools.partial(gram_kernel, ensemble=ensemble, per=per),
        in_specs=[VMEM] * 4,
        out_specs=[VMEM, HBM, VMEM],
        out_shape=[near(ensemble // 2 * PIECE, LANES), f32(ensemble, per * LANES), near(8, per * LANES)],
        scratch_shapes=[
            pltpu.VMEM((ensemble, per * LANES), jnp.float32),
            pltpu.SemaphoreType.DMA((per // 2,)),
        ],
        name="gram",
    )(in_vmem(rows), cell, value, var)


def piece_sum(pieces):
    return pl.pallas_call(
        piece_sum_kernel, in_specs=[VMEM], out_specs=VMEM, out_shape=near(*pieces.shape), name="piece_sum"
    )(in_vmem(pieces))


def analyse(pieces, dev, mean, ensemble, per):
    return pl.pallas_call(
        functools.partial(root_kernel, ensemble=ensemble, per=per),
        in_specs=[VMEM, HBM, VMEM],
        out_specs=VMEM,
        out_shape=near(ensemble * per, LANES),
        scratch_shapes=[
            pltpu.VMEM((len(SHIFT), ensemble, ensemble), jnp.float32),
            pltpu.VMEM((ensemble, per * LANES), jnp.float32),
            pltpu.SemaphoreType.DMA(()),
        ],
        name="analyse",
    )(in_vmem(pieces), dev, in_vmem(mean))


def advance(main, members, per):
    step = 8
    return pl.pallas_call(
        functools.partial(advance_kernel, members=step, per=per),
        grid=(members // step,),
        in_specs=[VMEM],
        out_specs=pl.BlockSpec((step, 3, 8, per // 3 * LANES), lambda i: (i, 0, 0, 0)),
        out_shape=f32(members, 3, 8, per // 3 * LANES),
        scratch_shapes=[pltpu.VMEM((UNROLL, per // 3 * 4, 24, LANES), jnp.float32)],
        cost_estimate=pl.CostEstimate(flops=1 << 28, transcendentals=0, bytes_accessed=1 << 22),
        name="advance",
    )(in_vmem(main))


def add_border(main, low, high, partial, members, per):
    step = 8
    block = pl.BlockSpec((step, 3, 8, per // 3 * LANES), lambda i: (i, 0, 0, 0))
    return pl.pallas_call(
        functools.partial(border_kernel, members=step, per=per),
        grid=(members // step,),
        in_specs=[pl.BlockSpec((8, step * per, LANES), lambda i: (0, i, 0)), VMEM, VMEM, block],
        out_specs=block,
        out_shape=f32(members, 3, 8, per // 3 * LANES),
        scratch_shapes=[pltpu.VMEM((UNROLL, per // 3 * 4, 24, LANES), jnp.float32)],
        input_output_aliases={3: 0},
        name="border",
    )(main.reshape(8, members * per, LANES), in_vmem(low), in_vmem(high), partial)


def exchange(rows, axes, count):
    moved = lax.all_to_all(rows.reshape(count, -1), axes, 0, 0, tiled=True)
    return moved.reshape(rows.shape)


def per_device(prior_mean_fields, ensemble_deviations, obs_cell, obs_value, obs_var):
    runners, tiles = lax.axis_size("runner"), lax.axis_size("tile")
    members_dev, _, _, width = ensemble_deviations.shape
    blocks = width // LANES
    per = 3 * blocks
    ensemble = members_dev * runners
    whole = ("runner", "tile")
    start = make_start(prior_mean_fields, ensemble_deviations)
    grids = exchange(start, "tile", tiles)
    forecast = runge_kutta(grids, tiles, members_dev // tiles, blocks)
    slab = exchange(forecast, whole, runners * tiles)
    pieces, dev, mean = gram_pieces(
        slab, obs_cell[0], obs_value[0], obs_var[0], ensemble, per
    )
    pieces = exchange(pieces, whole, runners * tiles)
    pieces = exchange(piece_sum(pieces), whole, runners * tiles)
    analysed = exchange(analyse(pieces, dev, mean, ensemble, per), "runner", runners)
    edge = 2 * members_dev * per
    forward = [(i, (i + 1) % tiles) for i in range(tiles)]
    backward = [(target, source) for source, target in forward]
    low = lax.ppermute(analysed[-edge:], "tile", forward)
    high = lax.ppermute(analysed[:edge], "tile", backward)
    partial = advance(analysed, members_dev, per)
    return add_border(analysed, low, high, partial, members_dev, per)


def solution(mesh):
    placed = (
        P(None, "tile", None),
        P("runner", None, "tile", None),
        P("tile", "runner", None),
        P("tile", "runner", None),
        P("tile", "runner", None),
    )
    return jax.shard_map(
        per_device,
        mesh=mesh,
        in_specs=placed,
        out_specs=P("runner", None, "tile", None),
        check_vma=False,
    )
```

```python
import functools
import math

import jax
import jax.numpy as jnp
from jax import lax
from jax.experimental import pallas as pl
from jax.experimental.pallas import tpu as pltpu
from jax.sharding import PartitionSpec as P

TIME_STEP = 0.25
CORIOLIS = 0.2
LANES = 128
ROOT2 = math.sqrt(2.0)
POLE_LOW = 3.0 - 2.0 * ROOT2
POLE_HIGH = 3.0 + 2.0 * ROOT2
SHIFT = (0.0, 1.0, POLE_LOW, POLE_HIGH)
ROOT_CONST = 0.125
ROOT_COEF = (
    0.125,
    0.5,
    2.0 * (1.0 - POLE_LOW) / (POLE_HIGH - POLE_LOW),
    2.0 * (POLE_HIGH - 1.0) / (POLE_HIGH - POLE_LOW),
)
BLOCK = 32
PANEL = 16
PIECE = 3


def start_kernel(prior_ref, dev_ref, out_ref):
    members, fields, rows, width = dev_ref.shape
    for m in range(members):
        for f in range(fields):
            for cb in range(width // LANES):
                at = ((m * fields + f) * (width // LANES) + cb) * rows
                lanes = slice(cb * LANES, (cb + 1) * LANES)
                out_ref[at : at + rows, :] = dev_ref[m, f, :, lanes] + prior_ref[f, :, lanes]


def roll_x(field, shift):
    return pltpu.roll(field, shift % field.shape[-1], axis=field.ndim - 1)


def along_x(field):
    return (roll_x(field, -1) - roll_x(field, 1)) - 0.125 * (roll_x(field, -2) - roll_x(field, 2))


def along_y(load, f):
    return (load(f, 1) - load(f, -1)) - 0.125 * (load(f, 2) - load(f, -2))


SLOPE = 8.0 / 12.0


def tendency(load):
    h, u, v = (load(f, 0) for f in range(3))
    height = -SLOPE * (along_x((1.0 + h) * u) + along_y(load, 3))
    east = CORIOLIS * v - SLOPE * (u * along_x(u) + v * along_y(load, 1) + along_x(h))
    north = -CORIOLIS * u - SLOPE * (u * along_x(v) + v * along_y(load, 2) + along_y(load, 0))
    return height, east, north


UNROLL = 4
RK_UNROLL = 16


def runge_kutta_kernel(in_ref, out_ref, even_ref, odd_ref, acc_ref, *, tiles, members, blocks):
    per = 3 * blocks
    grid_rows = tiles * 8
    sides = (even_ref, odd_ref)

    def split(value):
        return [value[:, cb * LANES : (cb + 1) * LANES] for cb in range(blocks)]

    def every_tile(step):
        def some(i, _):
            for r in range(RK_UNROLL):
                step(i * RK_UNROLL + r)
            return 0

        lax.fori_loop(0, tiles // RK_UNROLL, some, 0)

    def member_step(m, _):
        def start_of(t, f):
            return jnp.concatenate(
                [in_ref[pl.ds(((t * members + m) * per + f * blocks + cb) * 8, 8), :] for cb in range(blocks)],
                axis=1,
            )

        def put(ref, t, values):
            flux = (1.0 + values[0]) * values[2]
            for f, value in enumerate((*values, flux)):
                for cb, part in enumerate(split(value)):
                    ref[f * blocks + cb, pl.ds(8 + t * 8, 8), :] = part

        def wrap(ref):
            for j in range(4 * blocks):
                ref[j, 0:8, :] = ref[j, grid_rows : grid_rows + 8, :]
                ref[j, grid_rows + 8 : grid_rows + 16, :] = ref[j, 8:16, :]

        every_tile(lambda t: put(even_ref, t, [start_of(t, f) for f in range(3)]))
        wrap(even_ref)
        for stage in range(4):
            here, there = sides[stage % 2], sides[1 - stage % 2]

            def step(t, stage=stage, here=here, there=there):
                def load(f, shift):
                    return jnp.concatenate(
                        [here[f * blocks + cb, pl.ds(8 + t * 8 + shift, 8), :] for cb in range(blocks)],
                        axis=1,
                    )

                slopes = tendency(load)
                rows = pl.ds(t * 8, 8)
                nexts = []
                for f in range(3):
                    start = start_of(t, f)
                    weight = TIME_STEP / 6.0 * (1.0 if stage in (0, 3) else 2.0)
                    total = (start if stage == 0 else acc_ref[f, rows, :]) + weight * slopes[f]
                    if stage < 3:
                        acc_ref[f, rows, :] = total
                        nexts.append(start + TIME_STEP * (1.0 if stage == 2 else 0.5) * slopes[f])
                    else:
                        for cb, part in enumerate(split(total)):
                            at = t * (members * per) + m * per + f * blocks + cb
                            out_ref[pl.ds(at, 8, stride=tiles * members * per), :] = part
                if stage < 3:
                    put(there, t, nexts)

            every_tile(step)
            if stage < 3:
                wrap(there)
        return 0

    lax.fori_loop(0, members, member_step, 0)


def gram_kernel(
    in_ref, cell_ref, value_ref, var_ref, pack_ref, dev_ref, mean_ref, buf_ref, sem_ref, *, ensemble, per
):
    inverse = 1.0 / var_ref[...]
    count = inverse.shape[1]
    observed = jnp.concatenate(
        [cell_ref[...].astype(jnp.float32), inverse, value_ref[...] * inverse, jnp.zeros((5, count), jnp.float32)],
        axis=0,
    ).T
    cells, inv_var, val_w = (
        jnp.broadcast_to(observed[:, i : i + 1], (count, LANES)) for i in range(3)
    )
    cells = cells.astype(jnp.int32)
    copies = []
    lane = lax.broadcasted_iota(jnp.int32, (count, LANES), 1)
    total = jnp.zeros((ensemble + 8, ensemble), jnp.float32)
    for pair in range(per // 2):
        devs, lefts = [], []
        for j in (2 * pair, 2 * pair + 1):
            hit = cells == lane + j * LANES
            w = jnp.sum(jnp.where(hit, inv_var, 0.0), axis=0, keepdims=True)
            vw = jnp.sum(jnp.where(hit, val_w, 0.0), axis=0, keepdims=True)
            full = in_ref[pl.ds(j, ensemble, stride=per), :]
            mean = jnp.sum(full, axis=0, keepdims=True) * (1.0 / ensemble)
            dev = full - mean
            buf_ref[:, j * LANES : (j + 1) * LANES] = dev
            mean_ref[:, j * LANES : (j + 1) * LANES] = jnp.broadcast_to(mean, (8, LANES))
            devs.append(dev)
            z = jnp.broadcast_to(vw - mean * w, (8, LANES))
            lefts.append(jnp.concatenate([dev * w, z], axis=0))
        lanes = slice(pair * 2 * LANES, (pair + 1) * 2 * LANES)
        copies.append(pltpu.make_async_copy(buf_ref.at[:, lanes], dev_ref.at[:, lanes], sem_ref.at[pair]))
        copies[-1].start()
        x1, x2, x3 = split3(jnp.concatenate(lefts, axis=1))
        y1, y2, y3 = split3(jnp.concatenate(devs, axis=1))
        total = total + lax.dot_general(
            jnp.concatenate([x1, x1, x2, x2, x1, x3], axis=1),
            jnp.concatenate([y1, y2, y1, y2, y3, y1], axis=1),
            (((1,), (1,)), ((), ())),
            preferred_element_type=jnp.float32,
        )
    half = ensemble // 2
    sub = lax.broadcasted_iota(jnp.int32, (half, LANES), 0)
    col = lax.broadcasted_iota(jnp.int32, (half, LANES), 1)
    low, high = total[half:ensemble, LANES:], total[:half, :LANES]
    diagonal = jnp.sum(jnp.where(sub == col, low, 0.0), axis=0, keepdims=True)
    inn = total[ensemble : ensemble + 1, :]
    pack_ref[pl.ds(0, half, stride=PIECE), :] = total[:half, LANES:]
    pack_ref[pl.ds(1, half, stride=PIECE), :] = jnp.where(col >= sub, high, low)
    extra = jnp.zeros((half, LANES), jnp.float32)
    for i, row in enumerate((inn[:, :LANES], inn[:, LANES:], diagonal)):
        extra = jnp.where(sub == i, jnp.broadcast_to(row, (half, LANES)), extra)
    pack_ref[pl.ds(2, half, stride=PIECE), :] = extra
    for copy in copies:
        copy.wait()


def unpack_gram(ref, half):
    sub = lax.broadcasted_iota(jnp.int32, (half, LANES), 0)
    col = lax.broadcasted_iota(jnp.int32, (half, LANES), 1)
    cross = ref[pl.ds(0, half, stride=PIECE), :]
    both = ref[pl.ds(1, half, stride=PIECE), :]
    turned = both.T
    first = jnp.where(col >= sub, both, turned)
    second = jnp.where(col < sub, both, turned)
    second = jnp.where(col == sub, jnp.broadcast_to(ref[2 * PIECE + 2 : 2 * PIECE + 3, :], (half, LANES)), second)
    gram = jnp.concatenate(
        [jnp.concatenate([first, cross], axis=1), jnp.concatenate([cross.T, second], axis=1)], axis=0
    )
    innovation = jnp.concatenate([ref[2:3, :], ref[PIECE + 2 : PIECE + 3, :]], axis=1)
    return gram, innovation


def piece_sum_kernel(in_ref, out_ref):
    count = in_ref.shape[0] // PIECE
    for q in range(PIECE):
        total = jnp.sum(in_ref[pl.ds(q, count, stride=PIECE), :], axis=0, keepdims=True)
        out_ref[pl.ds(q, count, stride=PIECE), :] = jnp.broadcast_to(total, (count, LANES))


def split3(x):
    hi = x.astype(jnp.bfloat16)
    rest = x - hi.astype(jnp.float32)
    mid = rest.astype(jnp.bfloat16)
    low = (rest - mid.astype(jnp.float32)).astype(jnp.bfloat16)
    return hi, mid, low


def packed_inverse(packed, group):
    shape = (8, LANES)
    lane = lax.broadcasted_iota(jnp.int32, shape, 1)
    sub = lax.broadcasted_iota(jnp.int32, shape, 0)
    within = lane % group
    first = lane - within
    count = group // 8
    rows = [packed[8 * i : 8 * i + 8, :] for i in range(count)]

    def spread(parts, k):
        return jnp.broadcast_to(parts[k // 8][k % 8 : k % 8 + 1, :], shape)

    def sweep(parts, column, k, row):
        out = [part - c * row for part, c in zip(parts, column)]
        out[k // 8] = jnp.where(sub == k % 8, row, out[k // 8])
        return out

    for k0 in range(0, group, PANEL):
        panel = range(k0, k0 + PANEL)
        columns = {k: [jnp.take_along_axis(part, first + k, axis=1) for part in rows] for k in panel}
        for k in panel:
            column = columns.pop(k)
            inv = 1.0 / spread(column, k)
            for j in columns:
                columns[j] = sweep(columns[j], column, k, spread(columns[j], k) * inv)
            row = jnp.where(within == k, -1.0, spread(rows, k)) * inv
            rows = sweep([jnp.where(within == k, 0.0, part) for part in rows], column, k, row)
    return jnp.concatenate(rows, axis=0)


def root_kernel(in_ref, dev_ref, mean_ref, out_ref, work_ref, buf_ref, sem_ref, *, ensemble, per):
    fetch = pltpu.make_async_copy(dev_ref, buf_ref, sem_ref)
    fetch.start()
    half = ensemble // 2
    n = ensemble
    row_id = lax.broadcasted_iota(jnp.int32, (n, n), 0)
    lane_id = lax.broadcasted_iota(jnp.int32, (n, n), 1)
    diag = row_id == lane_id
    gram, innovation = unpack_gram(in_ref, half)
    matrix = gram * (1.0 / (ensemble - 1.0))
    for s, shift in enumerate(SHIFT):
        work_ref[s] = matrix + jnp.where(diag, 1.0 + shift, 0.0)
    shifts = len(SHIFT)
    lane_small = lax.broadcasted_iota(jnp.int32, (BLOCK, LANES), 1)
    lane_wide = lax.broadcasted_iota(jnp.int32, (BLOCK, n), 1)
    row_wide = lax.broadcasted_iota(jnp.int32, (BLOCK, n), 0)
    for k in range(n // BLOCK):
        rows = [work_ref[s, k * BLOCK : (k + 1) * BLOCK, :] for s in range(shifts)]
        near = (k * BLOCK) // LANES * LANES
        packed = jnp.zeros((BLOCK, LANES), jnp.float32)
        for s in range(shifts):
            move = (BLOCK * s - (k * BLOCK - near)) % LANES
            piece = rows[s][:, near : near + LANES]
            if move:
                piece = pltpu.roll(piece, move, axis=1)
            packed = jnp.where(lane_small // BLOCK == s, piece, packed)
        inverse = packed_inverse(packed, BLOCK)
        left = jnp.concatenate(
            [jnp.where(lane_small // BLOCK == s, -inverse, 0.0) for s in range(shifts)], axis=0
        )
        own = (lane_wide >= k * BLOCK) & (lane_wide < (k + 1) * BLOCK)
        minus_eye = jnp.where(lane_wide == row_wide + k * BLOCK, -1.0, 0.0)
        bars = [jnp.where(own, minus_eye, r) for r in rows]
        l1, l2, l3 = split3(left)
        b1, b2, b3 = split3(jnp.concatenate(bars, axis=0))
        swept = jnp.dot(
            jnp.concatenate([l1, l1, l2, l2, l1, l3], axis=1),
            jnp.concatenate([b1, b2, b1, b2, b3, b1], axis=0),
            preferred_element_type=jnp.float32,
        )
        own_all = (lane_id >= k * BLOCK) & (lane_id < (k + 1) * BLOCK)
        stacked = []
        for s in range(shifts):
            z = swept[s * BLOCK : (s + 1) * BLOCK, :]
            y1, y2, y3 = split3(jnp.where(own, 0.0, z))
            r1, r2, r3 = (b[s * BLOCK : (s + 1) * BLOCK, :] for b in (b1, b2, b3))
            stacked.append(
                (jnp.concatenate([y1, y1, y2, y2, y1, y3], axis=0), jnp.concatenate([r1, r2, r1, r2, r3, r1], axis=0))
            )
        ahead = (k + 1) * BLOCK // half % 2
        for side in (ahead, 1 - ahead):
            here = slice(side * half, (side + 1) * half)
            for s, (y, r) in enumerate(stacked):
                update = lax.dot_general(
                    y[:, here], r, (((0,), (0,)), ((), ())), preferred_element_type=jnp.float32
                )
                work_ref[s, here, :] = jnp.where(own_all[here], 0.0, work_ref[s, here, :]) - update
        for s in range(shifts):
            work_ref[s, k * BLOCK : (k + 1) * BLOCK, :] = swept[s * BLOCK : (s + 1) * BLOCK, :]
    root = jnp.where(diag, ROOT_CONST, 0.0)
    for s in range(shifts):
        root = root - ROOT_COEF[s] * work_ref[s]
    inner = jnp.sum(root * innovation, axis=1, keepdims=True)
    weights = jnp.sum(root * inner, axis=0, keepdims=True) * (1.0 / (ensemble - 1.0))
    mixing = root + weights
    m1, m2, m3 = split3(mixing)
    mixing6 = jnp.concatenate([m1, m1, m2, m2, m1, m3], axis=1)
    fetch.wait()
    for pair in range(per // 2):
        lanes = slice(pair * 2 * LANES, (pair + 1) * 2 * LANES)
        d1, d2, d3 = split3(buf_ref[:, lanes])
        mixed = mean_ref[0:1, lanes] + jnp.dot(
            mixing6, jnp.concatenate([d1, d2, d1, d2, d3, d1], axis=0), preferred_element_type=jnp.float32
        )
        for i in range(2):
            out_ref[pl.ds(2 * pair + i, ensemble, stride=per), :] = mixed[:, i * LANES : (i + 1) * LANES]


def each_member(one, members):
    def some(i, _):
        for r in range(UNROLL):
            one(i * UNROLL + r, r)
        return 0

    lax.fori_loop(0, members // UNROLL, some, 0)


def clear(buf_ref):
    @pl.when(pl.program_id(0) == 0)
    def _():
        buf_ref[...] = jnp.zeros(buf_ref.shape, jnp.float32)


def with_flux(parts, blocks):
    return parts + [(1.0 + parts[cb]) * parts[2 * blocks + cb] for cb in range(blocks)]


def loader(buf_ref, slot, blocks):
    def load(f, shift):
        return jnp.concatenate(
            [buf_ref[slot, f * blocks + cb, 8 + shift : 16 + shift, :] for cb in range(blocks)], axis=1
        )

    return load


def advance_kernel(main_ref, out_ref, north_ref, buf_ref, *, members, per):
    blocks = per // 3
    stride = main_ref.shape[0] // 8
    first = pl.program_id(0) * members
    clear(buf_ref)

    def one(i, slot):
        parts = [main_ref[pl.ds((first + i) * per + j, 8, stride=stride), :] for j in range(per)]
        for j, part in enumerate(with_flux(parts, blocks)):
            buf_ref[slot, j, 8:16, :] = part
        for cb in range(blocks):
            north_ref[i, cb] = parts[2 * blocks + cb]
        load = loader(buf_ref, slot, blocks)
        slopes = tendency(load)
        for f in range(3):
            out_ref[i, f] = load(f, 0) + TIME_STEP * slopes[f]

    each_member(one, members)


def border_kernel(north_ref, low_ref, high_ref, part_ref, out_ref, buf_ref, *, members, per):
    blocks = per // 3
    stride = low_ref.shape[0] // 2
    first = pl.program_id(0) * members
    clear(buf_ref)

    def one(i, slot):
        at = (first + i) * per
        for row, ref in ((6, low_ref), (16, high_ref)):
            parts = [ref[pl.ds(at + j, 2, stride=stride), :] for j in range(per)]
            for j, part in enumerate(with_flux(parts, blocks)):
                buf_ref[slot, j, row : row + 2, :] = part
        v = jnp.concatenate([north_ref[i, cb] for cb in range(blocks)], axis=1)
        load = loader(buf_ref, slot, blocks)
        rates = along_y(load, 3), v * along_y(load, 1), v * along_y(load, 2) + along_y(load, 0)
        for f in range(3):
            out_ref[i, f] = part_ref[i, f] - (TIME_STEP * SLOPE) * rates[f]

    each_member(one, members)


VMEM = pl.BlockSpec(memory_space=pltpu.VMEM)
HBM = pl.BlockSpec(memory_space=pl.ANY)


def f32(*shape):
    return jax.ShapeDtypeStruct(shape, jnp.float32)


def near(*shape):
    return pltpu.VMEM(shape, jnp.float32)


def in_vmem(x):
    return pltpu.with_memory_space_constraint(x, pltpu.VMEM)


def make_start(prior, deviations):
    members, fields, rows, width = deviations.shape
    step = 16
    return pl.pallas_call(
        start_kernel,
        grid=(members // step,),
        in_specs=[
            pl.BlockSpec((fields, rows, width), lambda i: (0, 0, 0)),
            pl.BlockSpec((step, fields, rows, width), lambda i: (i, 0, 0, 0)),
        ],
        out_specs=pl.BlockSpec((step * fields * rows * width // LANES, LANES), lambda i: (i, 0)),
        out_shape=near(members * fields * rows * width // LANES, LANES),
        name="start",
    )(prior, deviations)


def runge_kutta(rows, tiles, members, blocks):
    per = 3 * blocks
    return pl.pallas_call(
        functools.partial(runge_kutta_kernel, tiles=tiles, members=members, blocks=blocks),
        in_specs=[VMEM],
        out_specs=VMEM,
        out_shape=near(*rows.shape),
        scratch_shapes=[
            pltpu.VMEM((4 * blocks, tiles * 8 + 16, LANES), jnp.float32),
            pltpu.VMEM((4 * blocks, tiles * 8 + 16, LANES), jnp.float32),
            pltpu.VMEM((3, tiles * 8, blocks * LANES), jnp.float32),
        ],
        name="runge_kutta",
    )(in_vmem(rows))


def gram_pieces(rows, cell, value, var, ensemble, per):
    return pl.pallas_call(
        functools.partial(gram_kernel, ensemble=ensemble, per=per),
        in_specs=[VMEM] * 4,
        out_specs=[VMEM, HBM, VMEM],
        out_shape=[near(ensemble // 2 * PIECE, LANES), f32(ensemble, per * LANES), near(8, per * LANES)],
        scratch_shapes=[
            pltpu.VMEM((ensemble, per * LANES), jnp.float32),
            pltpu.SemaphoreType.DMA((per // 2,)),
        ],
        name="gram",
    )(in_vmem(rows), cell, value, var)


def piece_sum(pieces):
    return pl.pallas_call(
        piece_sum_kernel, in_specs=[VMEM], out_specs=VMEM, out_shape=near(*pieces.shape), name="piece_sum"
    )(in_vmem(pieces))


def analyse(pieces, dev, mean, ensemble, per):
    return pl.pallas_call(
        functools.partial(root_kernel, ensemble=ensemble, per=per),
        in_specs=[VMEM, HBM, VMEM],
        out_specs=VMEM,
        out_shape=near(ensemble * per, LANES),
        scratch_shapes=[
            pltpu.VMEM((len(SHIFT), ensemble, ensemble), jnp.float32),
            pltpu.VMEM((ensemble, per * LANES), jnp.float32),
            pltpu.SemaphoreType.DMA(()),
        ],
        name="analyse",
    )(in_vmem(pieces), dev, in_vmem(mean))


def advance(main, members, per):
    step = 8
    return pl.pallas_call(
        functools.partial(advance_kernel, members=step, per=per),
        grid=(members // step,),
        in_specs=[VMEM],
        out_specs=[
            pl.BlockSpec((step, 3, 8, per // 3 * LANES), lambda i: (i, 0, 0, 0)),
            pl.BlockSpec((step, per // 3, 8, LANES), lambda i: (i, 0, 0, 0)),
        ],
        out_shape=[f32(members, 3, 8, per // 3 * LANES), f32(members, per // 3, 8, LANES)],
        scratch_shapes=[pltpu.VMEM((UNROLL, per // 3 * 4, 24, LANES), jnp.float32)],
        cost_estimate=pl.CostEstimate(flops=1 << 28, transcendentals=0, bytes_accessed=1 << 22),
        name="advance",
    )(in_vmem(main))


def add_border(north, low, high, partial, members, per):
    step = 16
    block = pl.BlockSpec((step, 3, 8, per // 3 * LANES), lambda i: (i, 0, 0, 0))
    return pl.pallas_call(
        functools.partial(border_kernel, members=step, per=per),
        grid=(members // step,),
        in_specs=[pl.BlockSpec((step, per // 3, 8, LANES), lambda i: (i, 0, 0, 0)), VMEM, VMEM, block],
        out_specs=block,
        out_shape=f32(members, 3, 8, per // 3 * LANES),
        scratch_shapes=[pltpu.VMEM((UNROLL, per // 3 * 4, 24, LANES), jnp.float32)],
        input_output_aliases={3: 0},
        name="border",
    )(north, in_vmem(low), in_vmem(high), partial)


def exchange(rows, axes, count):
    moved = lax.all_to_all(rows.reshape(count, -1), axes, 0, 0, tiled=True)
    return moved.reshape(rows.shape)


def per_device(prior_mean_fields, ensemble_deviations, obs_cell, obs_value, obs_var):
    runners, tiles = lax.axis_size("runner"), lax.axis_size("tile")
    members_dev, _, _, width = ensemble_deviations.shape
    blocks = width // LANES
    per = 3 * blocks
    ensemble = members_dev * runners
    whole = ("runner", "tile")
    start = make_start(prior_mean_fields, ensemble_deviations)
    grids = exchange(start, "tile", tiles)
    forecast = runge_kutta(grids, tiles, members_dev // tiles, blocks)
    slab = exchange(forecast, whole, runners * tiles)
    pieces, dev, mean = gram_pieces(
        slab, obs_cell[0], obs_value[0], obs_var[0], ensemble, per
    )
    pieces = exchange(pieces, whole, runners * tiles)
    pieces = exchange(piece_sum(pieces), whole, runners * tiles)
    analysed = exchange(analyse(pieces, dev, mean, ensemble, per), "runner", runners)
    edge = 2 * members_dev * per
    forward = [(i, (i + 1) % tiles) for i in range(tiles)]
    backward = [(target, source) for source, target in forward]
    low = lax.ppermute(analysed[-edge:], "tile", forward)
    high = lax.ppermute(analysed[:edge], "tile", backward)
    partial, north = advance(analysed, members_dev, per)
    return add_border(north, low, high, partial, members_dev, per)


def solution(mesh):
    placed = (
        P(None, "tile", None),
        P("runner", None, "tile", None),
        P("tile", "runner", None),
        P("tile", "runner", None),
        P("tile", "runner", None),
    )
    return jax.shard_map(
        per_device,
        mesh=mesh,
        in_specs=placed,
        out_specs=P("runner", None, "tile", None),
        check_vma=False,
    )
```

```python
import functools
import math

import jax
import jax.numpy as jnp
from jax import lax
from jax.experimental import pallas as pl
from jax.experimental.pallas import tpu as pltpu
from jax.sharding import PartitionSpec as P

TIME_STEP = 0.25
CORIOLIS = 0.2
LANES = 128
ROOT2 = math.sqrt(2.0)
POLE_LOW = 3.0 - 2.0 * ROOT2
POLE_HIGH = 3.0 + 2.0 * ROOT2
SHIFT = (0.0, 1.0, POLE_LOW, POLE_HIGH)
ROOT_CONST = 0.125
ROOT_COEF = (
    0.125,
    0.5,
    2.0 * (1.0 - POLE_LOW) / (POLE_HIGH - POLE_LOW),
    2.0 * (POLE_HIGH - 1.0) / (POLE_HIGH - POLE_LOW),
)
BLOCK = 32
PANEL = 16
PIECE = 3


def start_kernel(prior_ref, dev_ref, out_ref):
    members, fields, rows, width = dev_ref.shape
    for m in range(members):
        for f in range(fields):
            for cb in range(width // LANES):
                at = ((m * fields + f) * (width // LANES) + cb) * rows
                lanes = slice(cb * LANES, (cb + 1) * LANES)
                out_ref[at : at + rows, :] = dev_ref[m, f, :, lanes] + prior_ref[f, :, lanes]


def roll_x(field, shift):
    return pltpu.roll(field, shift % field.shape[-1], axis=field.ndim - 1)


def along_x(field):
    return (roll_x(field, -1) - roll_x(field, 1)) - 0.125 * (roll_x(field, -2) - roll_x(field, 2))


def along_y(load, f):
    return (load(f, 1) - load(f, -1)) - 0.125 * (load(f, 2) - load(f, -2))


SLOPE = 8.0 / 12.0


def tendency(load):
    h, u, v = (load(f, 0) for f in range(3))
    height = -SLOPE * (along_x((1.0 + h) * u) + along_y(load, 3))
    east = CORIOLIS * v - SLOPE * (u * along_x(u) + v * along_y(load, 1) + along_x(h))
    north = -CORIOLIS * u - SLOPE * (u * along_x(v) + v * along_y(load, 2) + along_y(load, 0))
    return height, east, north


UNROLL = 8
RK_UNROLL = 16


def runge_kutta_kernel(in_ref, out_ref, even_ref, odd_ref, acc_ref, *, tiles, members, blocks):
    per = 3 * blocks
    grid_rows = tiles * 8
    sides = (even_ref, odd_ref)

    def split(value):
        return [value[:, cb * LANES : (cb + 1) * LANES] for cb in range(blocks)]

    def every_tile(step):
        def some(i, _):
            for r in range(RK_UNROLL):
                step(i * RK_UNROLL + r)
            return 0

        lax.fori_loop(0, tiles // RK_UNROLL, some, 0)

    def member_step(m, _):
        def start_of(t, f):
            return jnp.concatenate(
                [in_ref[pl.ds(((t * members + m) * per + f * blocks + cb) * 8, 8), :] for cb in range(blocks)],
                axis=1,
            )

        def put(ref, t, values):
            flux = (1.0 + values[0]) * values[2]
            for f, value in enumerate((*values, flux)):
                for cb, part in enumerate(split(value)):
                    ref[f * blocks + cb, pl.ds(8 + t * 8, 8), :] = part

        def wrap(ref):
            for j in range(4 * blocks):
                ref[j, 0:8, :] = ref[j, grid_rows : grid_rows + 8, :]
                ref[j, grid_rows + 8 : grid_rows + 16, :] = ref[j, 8:16, :]

        every_tile(lambda t: put(even_ref, t, [start_of(t, f) for f in range(3)]))
        wrap(even_ref)
        for stage in range(4):
            here, there = sides[stage % 2], sides[1 - stage % 2]

            def step(t, stage=stage, here=here, there=there):
                def load(f, shift):
                    return jnp.concatenate(
                        [here[f * blocks + cb, pl.ds(8 + t * 8 + shift, 8), :] for cb in range(blocks)],
                        axis=1,
                    )

                slopes = tendency(load)
                rows = pl.ds(t * 8, 8)
                nexts = []
                for f in range(3):
                    start = start_of(t, f)
                    weight = TIME_STEP / 6.0 * (1.0 if stage in (0, 3) else 2.0)
                    total = (start if stage == 0 else acc_ref[f, rows, :]) + weight * slopes[f]
                    if stage < 3:
                        acc_ref[f, rows, :] = total
                        nexts.append(start + TIME_STEP * (1.0 if stage == 2 else 0.5) * slopes[f])
                    else:
                        for cb, part in enumerate(split(total)):
                            at = t * (members * per) + m * per + f * blocks + cb
                            out_ref[pl.ds(at, 8, stride=tiles * members * per), :] = part
                if stage < 3:
                    put(there, t, nexts)

            every_tile(step)
            if stage < 3:
                wrap(there)
        return 0

    lax.fori_loop(0, members, member_step, 0)


def gram_kernel(
    in_ref, cell_ref, value_ref, var_ref, pack_ref, dev_ref, mean_ref, buf_ref, sem_ref, *, ensemble, per
):
    inverse = 1.0 / var_ref[...]
    count = inverse.shape[1]
    observed = jnp.concatenate(
        [cell_ref[...].astype(jnp.float32), inverse, value_ref[...] * inverse, jnp.zeros((5, count), jnp.float32)],
        axis=0,
    ).T
    cells, inv_var, val_w = (
        jnp.broadcast_to(observed[:, i : i + 1], (count, LANES)) for i in range(3)
    )
    cells = cells.astype(jnp.int32)
    copies = []
    lane = lax.broadcasted_iota(jnp.int32, (count, LANES), 1)
    total = jnp.zeros((ensemble + 8, ensemble), jnp.float32)
    for pair in range(per // 2):
        devs, lefts = [], []
        for j in (2 * pair, 2 * pair + 1):
            hit = cells == lane + j * LANES
            w = jnp.sum(jnp.where(hit, inv_var, 0.0), axis=0, keepdims=True)
            vw = jnp.sum(jnp.where(hit, val_w, 0.0), axis=0, keepdims=True)
            full = in_ref[pl.ds(j, ensemble, stride=per), :]
            mean = jnp.sum(full, axis=0, keepdims=True) * (1.0 / ensemble)
            dev = full - mean
            buf_ref[:, j * LANES : (j + 1) * LANES] = dev
            mean_ref[:, j * LANES : (j + 1) * LANES] = jnp.broadcast_to(mean, (8, LANES))
            devs.append(dev)
            z = jnp.broadcast_to(vw - mean * w, (8, LANES))
            lefts.append(jnp.concatenate([dev * w, z], axis=0))
        lanes = slice(pair * 2 * LANES, (pair + 1) * 2 * LANES)
        copies.append(pltpu.make_async_copy(buf_ref.at[:, lanes], dev_ref.at[:, lanes], sem_ref.at[pair]))
        copies[-1].start()
        x1, x2, x3 = split3(jnp.concatenate(lefts, axis=1))
        y1, y2, y3 = split3(jnp.concatenate(devs, axis=1))
        total = total + lax.dot_general(
            jnp.concatenate([x1, x1, x2, x2, x1, x3], axis=1),
            jnp.concatenate([y1, y2, y1, y2, y3, y1], axis=1),
            (((1,), (1,)), ((), ())),
            preferred_element_type=jnp.float32,
        )
    half = ensemble // 2
    sub = lax.broadcasted_iota(jnp.int32, (half, LANES), 0)
    col = lax.broadcasted_iota(jnp.int32, (half, LANES), 1)
    low, high = total[half:ensemble, LANES:], total[:half, :LANES]
    diagonal = jnp.sum(jnp.where(sub == col, low, 0.0), axis=0, keepdims=True)
    inn = total[ensemble : ensemble + 1, :]
    pack_ref[pl.ds(0, half, stride=PIECE), :] = total[:half, LANES:]
    pack_ref[pl.ds(1, half, stride=PIECE), :] = jnp.where(col >= sub, high, low)
    extra = jnp.zeros((half, LANES), jnp.float32)
    for i, row in enumerate((inn[:, :LANES], inn[:, LANES:], diagonal)):
        extra = jnp.where(sub == i, jnp.broadcast_to(row, (half, LANES)), extra)
    pack_ref[pl.ds(2, half, stride=PIECE), :] = extra
    for copy in copies:
        copy.wait()


def unpack_gram(ref, half):
    sub = lax.broadcasted_iota(jnp.int32, (half, LANES), 0)
    col = lax.broadcasted_iota(jnp.int32, (half, LANES), 1)
    cross = ref[pl.ds(0, half, stride=PIECE), :]
    both = ref[pl.ds(1, half, stride=PIECE), :]
    turned = both.T
    first = jnp.where(col >= sub, both, turned)
    second = jnp.where(col < sub, both, turned)
    second = jnp.where(col == sub, jnp.broadcast_to(ref[2 * PIECE + 2 : 2 * PIECE + 3, :], (half, LANES)), second)
    gram = jnp.concatenate(
        [jnp.concatenate([first, cross], axis=1), jnp.concatenate([cross.T, second], axis=1)], axis=0
    )
    innovation = jnp.concatenate([ref[2:3, :], ref[PIECE + 2 : PIECE + 3, :]], axis=1)
    return gram, innovation


def piece_sum_kernel(in_ref, out_ref):
    count = in_ref.shape[0] // PIECE
    for q in range(PIECE):
        total = jnp.sum(in_ref[pl.ds(q, count, stride=PIECE), :], axis=0, keepdims=True)
        out_ref[pl.ds(q, count, stride=PIECE), :] = jnp.broadcast_to(total, (count, LANES))


def split3(x):
    hi = x.astype(jnp.bfloat16)
    rest = x - hi.astype(jnp.float32)
    mid = rest.astype(jnp.bfloat16)
    low = (rest - mid.astype(jnp.float32)).astype(jnp.bfloat16)
    return hi, mid, low


def packed_inverse(packed, group):
    shape = (8, LANES)
    lane = lax.broadcasted_iota(jnp.int32, shape, 1)
    sub = lax.broadcasted_iota(jnp.int32, shape, 0)
    within = lane % group
    first = lane - within
    count = group // 8
    rows = [packed[8 * i : 8 * i + 8, :] for i in range(count)]

    def spread(parts, k):
        return jnp.broadcast_to(parts[k // 8][k % 8 : k % 8 + 1, :], shape)

    def sweep(parts, column, k, row):
        out = [part - c * row for part, c in zip(parts, column)]
        out[k // 8] = jnp.where(sub == k % 8, row, out[k // 8])
        return out

    for k0 in range(0, group, PANEL):
        panel = range(k0, k0 + PANEL)
        columns = {k: [jnp.take_along_axis(part, first + k, axis=1) for part in rows] for k in panel}
        for k in panel:
            column = columns.pop(k)
            inv = 1.0 / spread(column, k)
            for j in columns:
                columns[j] = sweep(columns[j], column, k, spread(columns[j], k) * inv)
            row = jnp.where(within == k, -1.0, spread(rows, k)) * inv
            rows = sweep([jnp.where(within == k, 0.0, part) for part in rows], column, k, row)
    return jnp.concatenate(rows, axis=0)


def root_kernel(in_ref, dev_ref, mean_ref, out_ref, work_ref, buf_ref, sem_ref, *, ensemble, per):
    fetch = pltpu.make_async_copy(dev_ref, buf_ref, sem_ref)
    fetch.start()
    half = ensemble // 2
    n = ensemble
    row_id = lax.broadcasted_iota(jnp.int32, (n, n), 0)
    lane_id = lax.broadcasted_iota(jnp.int32, (n, n), 1)
    diag = row_id == lane_id
    gram, innovation = unpack_gram(in_ref, half)
    matrix = gram * (1.0 / (ensemble - 1.0))
    for s, shift in enumerate(SHIFT):
        work_ref[s] = matrix + jnp.where(diag, 1.0 + shift, 0.0)
    shifts = len(SHIFT)
    lane_small = lax.broadcasted_iota(jnp.int32, (BLOCK, LANES), 1)
    lane_wide = lax.broadcasted_iota(jnp.int32, (BLOCK, n), 1)
    row_wide = lax.broadcasted_iota(jnp.int32, (BLOCK, n), 0)
    for k in range(n // BLOCK):
        rows = [work_ref[s, k * BLOCK : (k + 1) * BLOCK, :] for s in range(shifts)]
        near = (k * BLOCK) // LANES * LANES
        packed = jnp.zeros((BLOCK, LANES), jnp.float32)
        for s in range(shifts):
            move = (BLOCK * s - (k * BLOCK - near)) % LANES
            piece = rows[s][:, near : near + LANES]
            if move:
                piece = pltpu.roll(piece, move, axis=1)
            packed = jnp.where(lane_small // BLOCK == s, piece, packed)
        inverse = packed_inverse(packed, BLOCK)
        left = jnp.concatenate(
            [jnp.where(lane_small // BLOCK == s, -inverse, 0.0) for s in range(shifts)], axis=0
        )
        own = (lane_wide >= k * BLOCK) & (lane_wide < (k + 1) * BLOCK)
        minus_eye = jnp.where(lane_wide == row_wide + k * BLOCK, -1.0, 0.0)
        bars = [jnp.where(own, minus_eye, r) for r in rows]
        l1, l2, l3 = split3(left)
        b1, b2, b3 = split3(jnp.concatenate(bars, axis=0))
        swept = jnp.dot(
            jnp.concatenate([l1, l1, l2, l2, l1, l3], axis=1),
            jnp.concatenate([b1, b2, b1, b2, b3, b1], axis=0),
            preferred_element_type=jnp.float32,
        )
        own_all = (lane_id >= k * BLOCK) & (lane_id < (k + 1) * BLOCK)
        stacked = []
        for s in range(shifts):
            z = swept[s * BLOCK : (s + 1) * BLOCK, :]
            y1, y2, y3 = split3(jnp.where(own, 0.0, z))
            r1, r2, r3 = (b[s * BLOCK : (s + 1) * BLOCK, :] for b in (b1, b2, b3))
            stacked.append(
                (jnp.concatenate([y1, y1, y2, y2, y1, y3], axis=0), jnp.concatenate([r1, r2, r1, r2, r3, r1], axis=0))
            )
        ahead = (k + 1) * BLOCK // half % 2
        for side in (ahead, 1 - ahead):
            here = slice(side * half, (side + 1) * half)
            for s, (y, r) in enumerate(stacked):
                update = lax.dot_general(
                    y[:, here], r, (((0,), (0,)), ((), ())), preferred_element_type=jnp.float32
                )
                work_ref[s, here, :] = jnp.where(own_all[here], 0.0, work_ref[s, here, :]) - update
        for s in range(shifts):
            work_ref[s, k * BLOCK : (k + 1) * BLOCK, :] = swept[s * BLOCK : (s + 1) * BLOCK, :]
    root = jnp.where(diag, ROOT_CONST, 0.0)
    for s in range(shifts):
        root = root - ROOT_COEF[s] * work_ref[s]
    inner = jnp.sum(root * innovation, axis=1, keepdims=True)
    weights = jnp.sum(root * inner, axis=0, keepdims=True) * (1.0 / (ensemble - 1.0))
    mixing = root + weights
    m1, m2, m3 = split3(mixing)
    mixing6 = jnp.concatenate([m1, m1, m2, m2, m1, m3], axis=1)
    fetch.wait()
    for pair in range(per // 2):
        lanes = slice(pair * 2 * LANES, (pair + 1) * 2 * LANES)
        d1, d2, d3 = split3(buf_ref[:, lanes])
        mixed = mean_ref[0:1, lanes] + jnp.dot(
            mixing6, jnp.concatenate([d1, d2, d1, d2, d3, d1], axis=0), preferred_element_type=jnp.float32
        )
        for i in range(2):
            out_ref[pl.ds(2 * pair + i, ensemble, stride=per), :] = mixed[:, i * LANES : (i + 1) * LANES]


def each_member(one, members):
    def some(i, _):
        for r in range(UNROLL):
            one(i * UNROLL + r, r)
        return 0

    lax.fori_loop(0, members // UNROLL, some, 0)


def clear(buf_ref):
    @pl.when(pl.program_id(0) == 0)
    def _():
        buf_ref[...] = jnp.zeros(buf_ref.shape, jnp.float32)


def with_flux(parts, blocks):
    return parts + [(1.0 + parts[cb]) * parts[2 * blocks + cb] for cb in range(blocks)]


def loader(buf_ref, slot, blocks):
    def load(f, shift):
        return jnp.concatenate(
            [buf_ref[slot, f * blocks + cb, 8 + shift : 16 + shift, :] for cb in range(blocks)], axis=1
        )

    return load


def advance_kernel(main_ref, out_ref, north_ref, buf_ref, *, members, per):
    blocks = per // 3
    stride = main_ref.shape[0] // 8
    first = pl.program_id(0) * members
    clear(buf_ref)

    def one(i, slot):
        parts = [main_ref[pl.ds((first + i) * per + j, 8, stride=stride), :] for j in range(per)]
        for j, part in enumerate(with_flux(parts, blocks)):
            buf_ref[slot, j, 8:16, :] = part
        for cb in range(blocks):
            north_ref[i, cb] = parts[2 * blocks + cb]
        load = loader(buf_ref, slot, blocks)
        slopes = tendency(load)
        for f in range(3):
            out_ref[i, f] = load(f, 0) + TIME_STEP * slopes[f]

    each_member(one, members)


def border_kernel(north_ref, low_ref, high_ref, part_ref, out_ref, buf_ref, *, members, per):
    blocks = per // 3
    stride = low_ref.shape[0] // 2
    first = pl.program_id(0) * members
    clear(buf_ref)

    def one(i, slot):
        at = (first + i) * per
        for row, ref in ((6, low_ref), (16, high_ref)):
            parts = [ref[pl.ds(at + j, 2, stride=stride), :] for j in range(per)]
            for j, part in enumerate(with_flux(parts, blocks)):
                buf_ref[slot, j, row : row + 2, :] = part
        v = jnp.concatenate([north_ref[i, cb] for cb in range(blocks)], axis=1)
        load = loader(buf_ref, slot, blocks)
        rates = along_y(load, 3), v * along_y(load, 1), v * along_y(load, 2) + along_y(load, 0)
        for f in range(3):
            out_ref[i, f] = part_ref[i, f] - (TIME_STEP * SLOPE) * rates[f]

    each_member(one, members)


VMEM = pl.BlockSpec(memory_space=pltpu.VMEM)
HBM = pl.BlockSpec(memory_space=pl.ANY)


def f32(*shape):
    return jax.ShapeDtypeStruct(shape, jnp.float32)


def near(*shape):
    return pltpu.VMEM(shape, jnp.float32)


def in_vmem(x):
    return pltpu.with_memory_space_constraint(x, pltpu.VMEM)


def make_start(prior, deviations):
    members, fields, rows, width = deviations.shape
    step = 16
    return pl.pallas_call(
        start_kernel,
        grid=(members // step,),
        in_specs=[
            pl.BlockSpec((fields, rows, width), lambda i: (0, 0, 0)),
            pl.BlockSpec((step, fields, rows, width), lambda i: (i, 0, 0, 0)),
        ],
        out_specs=pl.BlockSpec((step * fields * rows * width // LANES, LANES), lambda i: (i, 0)),
        out_shape=near(members * fields * rows * width // LANES, LANES),
        name="start",
    )(prior, deviations)


def runge_kutta(rows, tiles, members, blocks):
    per = 3 * blocks
    return pl.pallas_call(
        functools.partial(runge_kutta_kernel, tiles=tiles, members=members, blocks=blocks),
        in_specs=[VMEM],
        out_specs=VMEM,
        out_shape=near(*rows.shape),
        scratch_shapes=[
            pltpu.VMEM((4 * blocks, tiles * 8 + 16, LANES), jnp.float32),
            pltpu.VMEM((4 * blocks, tiles * 8 + 16, LANES), jnp.float32),
            pltpu.VMEM((3, tiles * 8, blocks * LANES), jnp.float32),
        ],
        name="runge_kutta",
    )(in_vmem(rows))


def gram_pieces(rows, cell, value, var, ensemble, per):
    return pl.pallas_call(
        functools.partial(gram_kernel, ensemble=ensemble, per=per),
        in_specs=[VMEM] * 4,
        out_specs=[VMEM, HBM, VMEM],
        out_shape=[near(ensemble // 2 * PIECE, LANES), f32(ensemble, per * LANES), near(8, per * LANES)],
        scratch_shapes=[
            pltpu.VMEM((ensemble, per * LANES), jnp.float32),
            pltpu.SemaphoreType.DMA((per // 2,)),
        ],
        name="gram",
        compiler_params=pltpu.CompilerParams(),
    )(in_vmem(rows), cell, value, var)


def piece_sum(pieces):
    return pl.pallas_call(
        piece_sum_kernel, in_specs=[VMEM], out_specs=VMEM, out_shape=near(*pieces.shape), name="piece_sum"
    )(in_vmem(pieces))


def analyse(pieces, dev, mean, ensemble, per):
    return pl.pallas_call(
        functools.partial(root_kernel, ensemble=ensemble, per=per),
        in_specs=[VMEM, HBM, VMEM],
        out_specs=VMEM,
        out_shape=near(ensemble * per, LANES),
        scratch_shapes=[
            pltpu.VMEM((len(SHIFT), ensemble, ensemble), jnp.float32),
            pltpu.VMEM((ensemble, per * LANES), jnp.float32),
            pltpu.SemaphoreType.DMA(()),
        ],
        name="analyse",
        compiler_params=pltpu.CompilerParams(),
    )(in_vmem(pieces), dev, in_vmem(mean))


def advance(main, members, per):
    step = 8
    return pl.pallas_call(
        functools.partial(advance_kernel, members=step, per=per),
        grid=(members // step,),
        in_specs=[VMEM],
        out_specs=[
            pl.BlockSpec((step, 3, 8, per // 3 * LANES), lambda i: (i, 0, 0, 0)),
            pl.BlockSpec((step, per // 3, 8, LANES), lambda i: (i, 0, 0, 0)),
        ],
        out_shape=[f32(members, 3, 8, per // 3 * LANES), f32(members, per // 3, 8, LANES)],
        scratch_shapes=[pltpu.VMEM((UNROLL, per // 3 * 4, 24, LANES), jnp.float32)],
        cost_estimate=pl.CostEstimate(flops=1 << 28, transcendentals=0, bytes_accessed=1 << 22),
        name="advance",
    )(in_vmem(main))


def add_border(north, low, high, partial, members, per):
    step = 16
    block = pl.BlockSpec((step, 3, 8, per // 3 * LANES), lambda i: (i, 0, 0, 0))
    return pl.pallas_call(
        functools.partial(border_kernel, members=step, per=per),
        grid=(members // step,),
        in_specs=[pl.BlockSpec((step, per // 3, 8, LANES), lambda i: (i, 0, 0, 0)), VMEM, VMEM, block],
        out_specs=block,
        out_shape=f32(members, 3, 8, per // 3 * LANES),
        scratch_shapes=[pltpu.VMEM((UNROLL, per // 3 * 4, 24, LANES), jnp.float32)],
        input_output_aliases={3: 0},
        name="border",
    )(north, in_vmem(low), in_vmem(high), partial)


def exchange(rows, axes, count):
    moved = lax.all_to_all(rows.reshape(count, -1), axes, 0, 0, tiled=True)
    return moved.reshape(rows.shape)


def per_device(prior_mean_fields, ensemble_deviations, obs_cell, obs_value, obs_var):
    runners, tiles = lax.axis_size("runner"), lax.axis_size("tile")
    members_dev, _, _, width = ensemble_deviations.shape
    blocks = width // LANES
    per = 3 * blocks
    ensemble = members_dev * runners
    whole = ("runner", "tile")
    start = make_start(prior_mean_fields, ensemble_deviations)
    grids = exchange(start, "tile", tiles)
    forecast = runge_kutta(grids, tiles, members_dev // tiles, blocks)
    slab = exchange(forecast, whole, runners * tiles)
    pieces, dev, mean = gram_pieces(
        slab, obs_cell[0], obs_value[0], obs_var[0], ensemble, per
    )
    pieces = exchange(pieces, whole, runners * tiles)
    pieces = exchange(piece_sum(pieces), whole, runners * tiles)
    analysed = exchange(analyse(pieces, dev, mean, ensemble, per), "runner", runners)
    edge = 2 * members_dev * per
    forward = [(i, (i + 1) % tiles) for i in range(tiles)]
    backward = [(target, source) for source, target in forward]
    low = lax.ppermute(analysed[-edge:], "tile", forward)
    high = lax.ppermute(analysed[:edge], "tile", backward)
    partial, north = advance(analysed, members_dev, per)
    return add_border(north, low, high, partial, members_dev, per)


def solution(mesh):
    placed = (
        P(None, "tile", None),
        P("runner", None, "tile", None),
        P("tile", "runner", None),
        P("tile", "runner", None),
        P("tile", "runner", None),
    )
    return jax.shard_map(
        per_device,
        mesh=mesh,
        in_specs=placed,
        out_specs=P("runner", None, "tile", None),
        check_vma=False,
    )
```
